128 devices in a mesh: row: 8 (over y, core), col: 16 (over x, z).
Axes of the slice: x: 4, y: 4, z: 4, core: 2. Of those that a mesh axis runs over, the one named last changes fastest.
Arguments:
- obs_cell: int32 [128, 16, 128, 128], P(('row', 'col')), may hold values from 0 to 33554431, as said below
- obs_value: bfloat16 [128, 16, 128, 128], P(('row', 'col')), may hold values from -6 to 6
- obs_weight: bfloat16 [128, 16, 128, 128], P(('row', 'col')), may hold values from 0.5 to 2
- obs_count: int32 [128, 16, 128], P(('row', 'col')), may hold values from 0 to 128, as said below
- kappa_field: float32 [4096, 8192], P('row', 'col'), may hold values from 0.2 to 6
Outputs:
- solution_field: float32 [4096, 8192], P('row', 'col')
- residual: float32 [4096, 8192], P('row', 'col')
The draws below stay inside these ranges and needn't reach their ends.
Inputs may be any that keep to these rules, and one draw needn't show every extreme that they name: `obs_cell`: block (s, t, d) holds observations for tile t of device d, where device d is number d // 16 along row and d % (16) along col, and tile t is number t // 4 among the device's tiles along rows and t % (4) along columns, each tile 128 by 128 cells; every slot of the block, padding included, names a cell of that tile as row * 8192 + column. Slots at positions obs_count and beyond are padding. For one owner device, chosen afresh in each draw, every block from every source and tile is full.
All inputs are finite; a program needn't handle non-finite values.
Results may differ from the reference program's by a relative error of at most 0.0029.
Values may be sent and summed in bfloat16 or wider, within the bound.
A program may use at most 64 MiB of HBM per device.

```python
import math
import jax
import jax.numpy as jnp
from jax import lax

CR = 512
CC = 512
TILE = 128
BLOCK = 128
ITERS = 3
TILES = 16
NR = 4096
NC = 8192
DEVICES = 128


def draw_obs_count(key, part):
    key_pop, key_hot, key_load = jax.random.split(jax.random.fold_in(key, 11), 3)
    owners = jnp.arange(DEVICES, dtype=jnp.int32)
    popular = jax.random.randint(key_pop, (DEVICES,), 1, 5, dtype=jnp.int32)
    hottest = jax.random.randint(key_hot, (), 0, DEVICES, dtype=jnp.int32)
    popular = jnp.where(owners == hottest, 8, popular)
    raw_load = jax.random.randint(key_load, (DEVICES, TILES, DEVICES), 0, 2 * BLOCK + 1, dtype=jnp.int32)
    counts = jnp.minimum(BLOCK, raw_load * popular[None, None, :] // 4)
    counts = jnp.where(owners[None, None, :] == hottest, BLOCK, counts)
    return counts.astype(jnp.int32)


def draw_obs_cell(key, part):
    key_row, key_col = jax.random.split(jax.random.fold_in(key, 23))
    full_shape = (DEVICES, TILES, DEVICES, BLOCK)
    local_row = jax.random.randint(key_row, full_shape, 0, TILE, dtype=jnp.int32)
    local_col = jax.random.randint(key_col, full_shape, 0, TILE, dtype=jnp.int32)
    owners = jnp.arange(DEVICES, dtype=jnp.int32)[None, None, :, None]
    tile_ids = jnp.arange(TILES, dtype=jnp.int32)[None, :, None, None]
    grid_cols = NC // CC
    tile_span = CC // TILE
    lattice_row = owners // grid_cols * CR + tile_ids // tile_span * TILE + local_row
    lattice_col = owners % grid_cols * CC + tile_ids % tile_span * TILE + local_col
    return (lattice_row * NC + lattice_col).astype(jnp.int32)


def steps_of(own_key, extent, pieces, smallest, largest):
    def one(axis_at, shards_of):
        steps = jax.random.uniform(jax.random.fold_in(jax.random.fold_in(own_key, 6), axis_at), (shards_of,), jnp.float32, smallest / len(pieces), largest / len(pieces))
        return jnp.repeat(jnp.exp(steps), extent[axis_at] // shards_of).reshape((-1,) + (1,) * (len(extent) - axis_at - 1))

    gain = one(*pieces[0])
    for cut in pieces[1:]:
        gain = gain * one(*cut)
    return gain


def normal_values(key, extent, width, limit, cuts=(), held_as=jnp.bfloat16):
    array = jax.random.normal(key, extent, jnp.float32) * width
    if len(cuts) > 0:
        array = steps_of(key, extent, cuts, -0.22, 0.18) * array
    return jnp.clip(array, min=-limit, max=limit).astype(held_as)


def setup_inputs(seed: int = 0) -> dict:
    key_of = jax.random.split(jax.random.key(seed), 6)
    obs_cell = draw_obs_cell(jax.random.fold_in(key_of[5], 71), 0)
    obs_value = normal_values(key_of[1], (DEVICES, TILES, DEVICES, BLOCK), 1.0, 6.0, ((0, 128),))
    obs_weight = jnp.clip(jnp.exp(math.log(2.0) - 1.3862944 * jax.random.uniform(key_of[2], (DEVICES, TILES, DEVICES, BLOCK), jnp.float32) ** steps_of(key_of[2], (DEVICES, TILES, DEVICES, BLOCK), ((0, 128),), -0.2, 0.2)), 0.5, 2.0).astype(jnp.bfloat16)
    obs_count = draw_obs_count(jax.random.fold_in(key_of[5], 71), 0)
    kappa_field = jnp.clip(jnp.exp(math.log(6.0) - 3.4011974 * jax.random.uniform(key_of[4], (NR, NC), jnp.float32) ** steps_of(key_of[4], (NR, NC), ((0, 8), (1, 16)), -0.2, 0.2)), 0.2, 6.0)
    return {"obs_cell": obs_cell, "obs_value": obs_value, "obs_weight": obs_weight, "obs_count": obs_count, "kappa_field": kappa_field}


smooth_weight = 0.05


def stencil_step(field, kappa_field):
    padded = jnp.pad(field, 1)
    beside = padded[2:, 1:-1] + padded[:-2, 1:-1]
    beside = beside + padded[1:-1, 2:] + padded[1:-1, :-2]
    return (4.0 + kappa_field) * field - beside


def reference(obs_cell, obs_value, obs_weight, obs_count, kappa_field):
    rows_all, cols_all = kappa_field.shape
    positions = jnp.arange(BLOCK, dtype=jnp.int32)
    is_live = positions < obs_count[..., None]
    weight_wide = obs_weight.astype(jnp.float32)
    product = (weight_wide * obs_value.astype(jnp.float32)).astype(jnp.bfloat16)
    product = lax.optimization_barrier(product)
    masked_weight = jnp.where(is_live, weight_wide, jnp.float32(0.0)).reshape(-1)
    masked_resp = jnp.where(is_live, product.astype(jnp.float32), jnp.float32(0.0)).reshape(-1)
    flat_cells = obs_cell.reshape(-1).astype(jnp.int32)
    empty = jnp.zeros((rows_all * cols_all,), jnp.float32)
    weight_field = empty.at[flat_cells].add(masked_weight).reshape(rows_all, cols_all)
    response = empty.at[flat_cells].add(masked_resp).reshape(rows_all, cols_all)

    def operate(field):
        inner = stencil_step(field, kappa_field)
        return weight_field * field + smooth_weight * stencil_step(inner, kappa_field)

    solution_field = jnp.zeros_like(response)
    residual, direction = response, response
    norm_now = jnp.sum(residual * residual)
    for step in range(ITERS):
        image = operate(direction)
        alpha = norm_now / jnp.sum(direction * image)
        solution_field = solution_field + alpha * direction
        residual = residual - alpha * image
        norm_next = jnp.sum(residual * residual)
        direction = residual + (norm_next / norm_now) * direction
        norm_now = norm_next
    return solution_field, residual
```

```python
import functools

import jax
import jax.numpy as jnp
from jax import lax
from jax.experimental import pallas as pl
from jax.experimental.pallas import tpu as pltpu
from jax.sharding import PartitionSpec as P

TILE = 128
ITERS = 3
ROW = "row"
COL = "col"
MESH = pl.DeviceIdType.MESH
BF = jnp.bfloat16
F32 = jnp.float32
PITCH = 136
STRIDE = 5

smooth_weight = 0.05


def partner(row, col, rows, cols, k):
    devices = rows * cols
    q = (row * cols + col + (k * STRIDE) % devices) % devices
    return q // cols, q % cols


def source(row, col, rows, cols, k):
    devices = rows * cols
    q = (row * cols + col + devices - (k * STRIDE) % devices) % devices
    return q // cols, q % cols


def exchange_and_bin(
    rows, cols, cell_ref, value_ref, weight_ref, count_ref, wf_ref, resp_ref,
    stage_c, stage_w, stage_p, send_c, send_v, got_c, got_v,
    low_s, w_s, p_s, high_t, sent_c, sent_v, came_c, came_v,
):
    devices = rows * cols
    tiles = cell_ref.shape[0]
    row, col = lax.axis_index(ROW), lax.axis_index(COL)
    barrier = pltpu.get_barrier_semaphore()

    def greet(k, _):
        pr, pc = partner(row, col, rows, cols, k)
        pl.semaphore_signal(barrier, inc=1, device_id=(pr, pc), device_id_type=MESH)
        return 0

    lax.fori_loop(1, devices, greet, 0)

    counts = count_ref[...].T
    slot = lax.broadcasted_iota(jnp.int32, (devices, TILE), 1)
    for t in range(tiles):
        live = slot < jnp.broadcast_to(counts[:, t : t + 1], (devices, TILE))
        cell = cell_ref[t]
        code = jnp.bitwise_and(jnp.right_shift(cell, 13 + 6), 1) * 128 + jnp.bitwise_and(cell, 127)
        code = code * 64 + jnp.bitwise_and(jnp.right_shift(cell, 13), 63)
        wide = weight_ref[t].astype(F32)
        product = (wide * value_ref[t].astype(F32)).astype(BF).astype(F32)
        stage_c[pl.ds(t * PITCH, devices), :] = code
        stage_w[pl.ds(t * PITCH, devices), :] = jnp.where(live, wide, 0.0)
        stage_p[pl.ds(t * PITCH, devices), :] = jnp.where(live, product, 0.0)

    def gather(k, _):
        pr, pc = partner(row, col, rows, cols, k)
        q = pr * cols + pc
        rows_at = pl.ds(q, tiles, stride=PITCH)
        send_c[k] = stage_c[rows_at, :].astype(jnp.int16)
        send_v[k, 0:16, :] = stage_w[rows_at, :].astype(BF)
        send_v[k, 16:32, :] = stage_p[rows_at, :].astype(BF)
        return 0

    lax.fori_loop(0, devices, gather, 0)
    pl.semaphore_wait(barrier, devices - 1)

    def send(k, _):
        pr, pc = partner(row, col, rows, cols, k)
        pltpu.make_async_remote_copy(
            send_c.at[k], got_c.at[k], sent_c, came_c.at[k // 8],
            device_id=(pr, pc), device_id_type=MESH,
        ).start()
        pltpu.make_async_remote_copy(
            send_v.at[k], got_v.at[k], sent_v, came_v.at[k // 8],
            device_id=(pr, pc), device_id_type=MESH,
        ).start()
        return 0

    lax.fori_loop(1, devices, send, 0)
    got_c[0] = send_c[0]
    got_v[0] = send_v[0]
    wf_ref[...] = jnp.zeros_like(wf_ref)
    resp_ref[...] = jnp.zeros_like(resp_ref)

    lanes = lax.broadcasted_iota(jnp.int32, (16, 128), 1).astype(F32)
    high_ids = [lanes.astype(BF), (lanes + 128.0).astype(BF)]
    subs = lax.broadcasted_iota(jnp.int32, (16, 128), 0).astype(F32)
    low_ids = [(subs + 16.0 * g).astype(BF) for g in range(4)]
    one, zero = jnp.ones((16, 128), BF), jnp.zeros((16, 128), BF)
    across = wf_ref.shape[1] // TILE

    def bin_group(g):
        code = got_c[pl.ds(g * 8, 8)].reshape(128, 128).astype(jnp.int32)
        low_s[...] = jnp.bitwise_and(code, 63).astype(F32)
        high_t[...] = jnp.right_shift(code, 6).astype(F32).T
        for s in range(8):
            w_s[pl.ds(s * 16, 16), :] = got_v[g * 8 + s, 0:16, :].astype(F32)
            p_s[pl.ds(s * 16, 16), :] = got_v[g * 8 + s, 16:32, :].astype(F32)
        for t in range(tiles):
            total = None
            for pair in range(4):
                left, right = [], []
                for s in (2 * pair, 2 * pair + 1):
                    r = s * 16 + t
                    low, w, p = (
                        jnp.broadcast_to(ref[pl.ds(r, 1), :], (16, 128)).astype(BF)
                        for ref in (low_s, w_s, p_s)
                    )
                    hits = [low == ids for ids in low_ids]
                    left.append(
                        jnp.concatenate(
                            [jnp.where(h, w, zero) for h in hits]
                            + [jnp.where(h, p, zero) for h in hits],
                            axis=0,
                        )
                    )
                    high = jnp.broadcast_to(high_t[:, r : r + 1], (128, 128)).astype(BF)
                    for v in range(8):
                        part = high[16 * v : 16 * v + 16]
                        right.append(
                            jnp.concatenate([jnp.where(part == ids, one, zero) for ids in high_ids], axis=1)
                        )
                piece = jnp.dot(
                    jnp.concatenate(left, axis=1),
                    jnp.concatenate(right, axis=0),
                    preferred_element_type=F32,
                )
                total = piece if total is None else total + piece
            for ref, at in ((wf_ref, 0), (resp_ref, 64)):
                for half in range(2):
                    where = (
                        pl.ds((t // across) * TILE + half * 64, 64),
                        pl.ds((t % across) * TILE, TILE),
                    )
                    ref[where] = ref[where] + total[at : at + 64, half * 128 : half * 128 + 128]

    def arrived(first, size, g):
        there = pl.ds(first, size)
        pltpu.make_async_copy(got_c.at[there], got_c.at[there], came_c.at[g]).wait()
        pltpu.make_async_copy(got_v.at[there], got_v.at[there], came_v.at[g]).wait()

    def step(g, _):
        @pl.when(g == 0)
        def _():
            arrived(1, 7, 0)

        @pl.when(g > 0)
        def _():
            arrived(g * 8, 8, g)

        bin_group(g)
        return 0

    lax.fori_loop(0, devices // 8, step, 0)
    out = pl.ds(1, devices - 1)
    pltpu.make_async_copy(send_c.at[out], send_c.at[out], sent_c).wait()
    pltpu.make_async_copy(send_v.at[out], send_v.at[out], sent_v).wait()


def fields(rows, cols, obs_cell, obs_value, obs_weight, obs_count, shape):
    devices = rows * cols
    tiles = obs_cell.shape[0]
    vmem = pl.BlockSpec(memory_space=pltpu.VMEM)
    stage = (tiles * PITCH, TILE)
    return pl.pallas_call(
        functools.partial(exchange_and_bin, rows, cols),
        out_shape=[jax.ShapeDtypeStruct(shape, F32)] * 2,
        in_specs=[vmem] * 4,
        out_specs=[vmem] * 2,
        scratch_shapes=[
            pltpu.VMEM(stage, jnp.int32),
            pltpu.VMEM(stage, F32),
            pltpu.VMEM(stage, F32),
            pltpu.VMEM((devices, tiles, TILE), jnp.int16),
            pltpu.VMEM((devices, 2 * tiles, TILE), BF),
            pltpu.VMEM((devices, tiles, TILE), jnp.int16),
            pltpu.VMEM((devices, 2 * tiles, TILE), BF),
            pltpu.VMEM((128, 128), F32),
            pltpu.VMEM((128, 128), F32),
            pltpu.VMEM((128, 128), F32),
            pltpu.VMEM((128, 128), F32),
            pltpu.SemaphoreType.DMA,
            pltpu.SemaphoreType.DMA,
            pltpu.SemaphoreType.DMA((devices // 8,)),
            pltpu.SemaphoreType.DMA((devices // 8,)),
        ],
        name="exchange_and_bin",
        compiler_params=pltpu.CompilerParams(collective_id=0, has_side_effects=True),
    )(obs_cell, obs_value, obs_weight, obs_count)


def extended(x, sides, width):
    edges = {}
    for axis, dim in sides:
        size, length = (lax.axis_size(axis), x.shape[dim])
        up = [(i, (i + 1) % size) for i in range(size - 1)]
        last = lax.slice_in_dim(x, length - width, length, axis=dim)
        leading = lax.slice_in_dim(x, 0, width, axis=dim)
        edges[dim] = (
            lax.ppermute(last, axis, up),
            lax.ppermute(leading, axis, [(b, a) for a, b in up]),
        )
    done = []
    for _, dim in sides:
        low, high = edges[dim]
        around = [(width, width) if d in done else (0, 0) for d in range(x.ndim)]
        x = jnp.concatenate([jnp.pad(low, around), x, jnp.pad(high, around)], axis=dim)
        done.append(dim)
    return x


def one_axis_at_a_time(x, axes):
    return functools.reduce(lax.psum, axes, x)


def stencil_step(padded, kappa_field):
    center = padded[1:-1, 1:-1]
    beside = padded[2:, 1:-1] + padded[:-2, 1:-1]
    beside = beside + padded[1:-1, 2:] + padded[1:-1, :-2]
    return (4.0 + kappa_field) * center - beside


def per_device(obs_cell, obs_value, obs_weight, obs_count, kappa_field):
    rows, cols = lax.axis_size(ROW), lax.axis_size(COL)
    weight_field, response = fields(
        rows, cols, obs_cell[0], obs_value[0], obs_weight[0], obs_count[0], kappa_field.shape
    )

    def operate(field):
        first = extended(field, ((ROW, 0), (COL, 1)), 1)
        inner = stencil_step(first, kappa_field)
        second = extended(inner, ((ROW, 0), (COL, 1)), 1)
        return weight_field * field + smooth_weight * stencil_step(second, kappa_field)

    solution_field = jnp.zeros_like(response)
    residual = response

    def two_products(current, image):
        return (
            one_axis_at_a_time(jnp.sum(current * current), (ROW, COL)),
            one_axis_at_a_time(jnp.sum(current * image), (ROW, COL)),
        )

    image = operate(residual)
    norm_now, curvature = two_products(residual, image)
    alpha = norm_now / curvature
    direction, along = (residual, image)
    for step in range(ITERS):
        solution_field = solution_field + alpha * direction
        residual = residual - alpha * along
        if step + 1 < ITERS:
            image = operate(residual)
            norm_next, curvature = two_products(residual, image)
            ratio = norm_next / norm_now
            alpha = norm_next / (curvature - ratio * norm_next / alpha)
            direction = residual + ratio * direction
            along = image + ratio * along
            norm_now = norm_next
    return (solution_field, residual)


def solution(mesh):
    placed = (
        P((ROW, COL), None, None, None),
        P((ROW, COL), None, None, None),
        P((ROW, COL), None, None, None),
        P((ROW, COL), None, None),
        P(ROW, COL),
    )
    return jax.shard_map(
        per_device,
        mesh=mesh,
        in_specs=placed,
        out_specs=(P(ROW, COL), P(ROW, COL)),
        check_vma=False,
    )
```

```python
import functools

import jax
import jax.numpy as jnp
from jax import lax
from jax.experimental import pallas as pl
from jax.experimental.pallas import tpu as pltpu
from jax.sharding import PartitionSpec as P

TILE = 128
ITERS = 3
ROW = "row"
COL = "col"
MESH = pl.DeviceIdType.MESH
BF = jnp.bfloat16
F32 = jnp.float32
PITCH = 136
STRIDE = 5

smooth_weight = 0.05

SCALE = 1.0 / 256.0
SHIFT = 5.0
GROWTH_MAX = 1000.0
EDGE = 8
TOP = 16
WIDE = 128


def partner(row, col, rows, cols, k):
    devices = rows * cols
    q = (row * cols + col + (k * STRIDE) % devices) % devices
    return q // cols, q % cols


def source(row, col, rows, cols, k):
    devices = rows * cols
    q = (row * cols + col + devices - (k * STRIDE) % devices) % devices
    return q // cols, q % cols


def exchange_and_bin(
    rows, cols, cell_ref, value_ref, weight_ref, count_ref, wf_ref, resp_ref,
    stage_c, stage_w, stage_p, send_c, send_v, got_c, got_v,
    low_s, w_s, p_s, high_t, sent_c, sent_v, came_c, came_v,
):
    devices = rows * cols
    tiles = cell_ref.shape[0]
    row, col = lax.axis_index(ROW), lax.axis_index(COL)
    barrier = pltpu.get_barrier_semaphore()

    def greet(k, _):
        pr, pc = partner(row, col, rows, cols, k)
        pl.semaphore_signal(barrier, inc=1, device_id=(pr, pc), device_id_type=MESH)
        return 0

    lax.fori_loop(1, devices, greet, 0)

    counts = count_ref[...].T
    slot = lax.broadcasted_iota(jnp.int32, (devices, TILE), 1)
    for t in range(tiles):
        live = slot < jnp.broadcast_to(counts[:, t : t + 1], (devices, TILE))
        cell = cell_ref[t]
        code = jnp.bitwise_and(jnp.right_shift(cell, 13 + 6), 1) * 128 + jnp.bitwise_and(cell, 127)
        code = code * 64 + jnp.bitwise_and(jnp.right_shift(cell, 13), 63)
        wide = weight_ref[t].astype(F32)
        product = (wide * value_ref[t].astype(F32)).astype(BF).astype(F32)
        stage_c[pl.ds(t * PITCH, devices), :] = code
        stage_w[pl.ds(t * PITCH, devices), :] = jnp.where(live, wide, 0.0)
        stage_p[pl.ds(t * PITCH, devices), :] = jnp.where(live, product, 0.0)

    def gather(k, _):
        pr, pc = partner(row, col, rows, cols, k)
        q = pr * cols + pc
        rows_at = pl.ds(q, tiles, stride=PITCH)
        send_c[k] = stage_c[rows_at, :].astype(jnp.int16)
        send_v[k, 0:16, :] = stage_w[rows_at, :].astype(BF)
        send_v[k, 16:32, :] = stage_p[rows_at, :].astype(BF)
        return 0

    lax.fori_loop(0, devices, gather, 0)
    pl.semaphore_wait(barrier, devices - 1)

    def send(k, _):
        pr, pc = partner(row, col, rows, cols, k)
        pltpu.make_async_remote_copy(
            send_c.at[k], got_c.at[k], sent_c, came_c.at[k // 8],
            device_id=(pr, pc), device_id_type=MESH,
        ).start()
        pltpu.make_async_remote_copy(
            send_v.at[k], got_v.at[k], sent_v, came_v.at[k // 8],
            device_id=(pr, pc), device_id_type=MESH,
        ).start()
        return 0

    lax.fori_loop(1, devices, send, 0)
    got_c[0] = send_c[0]
    got_v[0] = send_v[0]
    wf_ref[...] = jnp.zeros_like(wf_ref)
    resp_ref[...] = jnp.zeros_like(resp_ref)

    lanes = lax.broadcasted_iota(jnp.int32, (16, 128), 1).astype(F32)
    high_ids = [lanes.astype(BF), (lanes + 128.0).astype(BF)]
    subs = lax.broadcasted_iota(jnp.int32, (16, 128), 0).astype(F32)
    low_ids = [(subs + 16.0 * g).astype(BF) for g in range(4)]
    one, zero = jnp.ones((16, 128), BF), jnp.zeros((16, 128), BF)
    across = wf_ref.shape[1] // TILE

    def bin_group(g):
        code = got_c[pl.ds(g * 8, 8)].reshape(128, 128).astype(jnp.int32)
        low_s[...] = jnp.bitwise_and(code, 63).astype(F32)
        high_t[...] = jnp.right_shift(code, 6).astype(F32).T
        for s in range(8):
            w_s[pl.ds(s * 16, 16), :] = got_v[g * 8 + s, 0:16, :].astype(F32)
            p_s[pl.ds(s * 16, 16), :] = got_v[g * 8 + s, 16:32, :].astype(F32)
        for t in range(tiles):
            total = None
            for pair in range(4):
                left, right = [], []
                for s in (2 * pair, 2 * pair + 1):
                    r = s * 16 + t
                    low, w, p = (
                        jnp.broadcast_to(ref[pl.ds(r, 1), :], (16, 128)).astype(BF)
                        for ref in (low_s, w_s, p_s)
                    )
                    hits = [low == ids for ids in low_ids]
                    left.append(
                        jnp.concatenate(
                            [jnp.where(h, w, zero) for h in hits]
                            + [jnp.where(h, p, zero) for h in hits],
                            axis=0,
                        )
                    )
                    high = jnp.broadcast_to(high_t[:, r : r + 1], (128, 128)).astype(BF)
                    for v in range(8):
                        part = high[16 * v : 16 * v + 16]
                        right.append(
                            jnp.concatenate([jnp.where(part == ids, one, zero) for ids in high_ids], axis=1)
                        )
                piece = jnp.dot(
                    jnp.concatenate(left, axis=1),
                    jnp.concatenate(right, axis=0),
                    preferred_element_type=F32,
                )
                total = piece if total is None else total + piece
            for ref, at in ((wf_ref, 0), (resp_ref, 64)):
                for half in range(2):
                    where = (
                        pl.ds((t // across) * TILE + half * 64, 64),
                        pl.ds((t % across) * TILE, TILE),
                    )
                    ref[where] = ref[where] + total[at : at + 64, half * 128 : half * 128 + 128]

    def arrived(first, size, g):
        there = pl.ds(first, size)
        pltpu.make_async_copy(got_c.at[there], got_c.at[there], came_c.at[g]).wait()
        pltpu.make_async_copy(got_v.at[there], got_v.at[there], came_v.at[g]).wait()

    def step(g, _):
        @pl.when(g == 0)
        def _():
            arrived(1, 7, 0)

        @pl.when(g > 0)
        def _():
            arrived(g * 8, 8, g)

        bin_group(g)
        return 0

    lax.fori_loop(0, devices // 8, step, 0)
    out = pl.ds(1, devices - 1)
    pltpu.make_async_copy(send_c.at[out], send_c.at[out], sent_c).wait()
    pltpu.make_async_copy(send_v.at[out], send_v.at[out], sent_v).wait()


def solve(m):
    shift = SCALE * SHIFT

    def at(p, i):
        return p[i] if 0 <= i < len(p) else None

    def plus(a, b):
        return b if a is None else a if b is None else a + b

    def dot(a, b):
        total, size = None, None
        for i, x in enumerate(a):
            for j, y in enumerate(b):
                term = x * y * m[i + j]
                total, size = plus(total, term), plus(size, jnp.abs(term))
        return total, size / jnp.abs(total)

    def times_a(p):
        out = []
        for i in range(len(p) + 1):
            scaled = None if at(p, i) is None else shift * p[i]
            out.append(plus(scaled, at(p, i - 1)))
        return out

    def axpy(a, b, c):
        return [
            plus(at(a, i), None if at(b, i) is None else c * b[i]) for i in range(max(len(a), len(b)))
        ]

    one = jnp.ones_like(m[0])
    x, r, p, rr, growth = [], [one], [one], m[0], one
    for step in range(ITERS):
        ap = times_a(p)
        pap, grown = dot(p, ap)
        growth = jnp.where(grown <= growth, growth, grown)
        alpha = rr / pap
        x, r = axpy(x, p, alpha), axpy(r, ap, -alpha)
        if step + 1 < ITERS:
            new, grown = dot(r, r)
            growth = jnp.where(grown <= growth, growth, grown)
            p, rr = axpy(r, p, new / rr), new
    return x, r, growth


def smooth(
    rows, cols, kappa_ref, wf_ref, resp_ref, x_ref, r_ref, growth_ref,
    v0, v1, v2, v3, u, w, c, send_rows, send_cols, got_rows, got_cols, got_corners,
    part, parts, sent_edge, came_edge, sent_part, came_part,
):
    devices = rows * cols
    high, wide = kappa_ref.shape
    row, col = lax.axis_index(ROW), lax.axis_index(COL)
    me = row * cols + col
    above, below = (row + rows - 1) % rows, (row + 1) % rows
    before, after = (col + cols - 1) % cols, (col + 1) % cols
    has_above = jnp.where(row > 0, 1.0, 0.0).astype(F32)
    has_below = jnp.where(row < rows - 1, 1.0, 0.0).astype(F32)
    has_before = jnp.where(col > 0, 1.0, 0.0).astype(F32)
    has_after = jnp.where(col < cols - 1, 1.0, 0.0).astype(F32)
    tall = high + 2 * TOP
    full = wide + WIDE
    own_rows, own_cols = pl.ds(TOP, high), pl.ds(0, wide)

    fields = (v0, w, c)
    for ref in (v0, w, c, u, v1, v2):
        ref[pl.ds(0, TOP), :] = jnp.zeros((TOP, full), F32)
        ref[pl.ds(TOP + high, TOP), :] = jnp.zeros((TOP, full), F32)
    v0[own_rows, own_cols] = resp_ref[...]
    w[own_rows, own_cols] = (wf_ref[...] - SHIFT) * SCALE
    c[own_rows, own_cols] = kappa_ref[...] + 4.0
    lane = lax.broadcasted_iota(jnp.int32, (WIDE, WIDE), 1)
    for f, ref in enumerate(fields):
        send_rows[0, f] = ref[pl.ds(TOP, EDGE), own_cols]
        send_rows[1, f] = ref[pl.ds(TOP + high - EDGE, EDGE), own_cols]
        for i in range(high // WIDE):
            block = pl.ds(TOP + i * WIDE, WIDE)
            left = ref[block, pl.ds(0, WIDE)]
            right = ref[block, pl.ds(wide - WIDE, WIDE)]
            turned = jnp.where(lane < 64, left, right).T
            send_cols[0, f, :, pl.ds(i * WIDE, WIDE)] = turned[0:EDGE]
            send_cols[1, f, :, pl.ds(i * WIDE, WIDE)] = turned[WIDE - EDGE :]

    def copies():
        first, last = pl.ds(0, WIDE), pl.ds(high - WIDE, WIDE)
        plan = [
            (send_rows.at[0], got_rows.at[1], above, col),
            (send_rows.at[1], got_rows.at[0], below, col),
            (send_cols.at[0], got_cols.at[1], row, before),
            (send_cols.at[1], got_cols.at[0], row, after),
            (send_cols.at[0, :, :, first], got_corners.at[3], above, before),
            (send_cols.at[0, :, :, last], got_corners.at[1], below, before),
            (send_cols.at[1, :, :, first], got_corners.at[2], above, after),
            (send_cols.at[1, :, :, last], got_corners.at[0], below, after),
        ]
        return [
            pltpu.make_async_remote_copy(
                source, target, sent_edge.at[i], came_edge.at[i], device_id=(pr, pc), device_id_type=MESH
            )
            for i, (source, target, pr, pc) in enumerate(plan)
        ]

    edges = copies()
    for copy in edges:
        copy.start()
    for copy in edges:
        copy.wait()
    gap = jnp.zeros((WIDE - 2 * EDGE, WIDE), F32)
    for f, ref in enumerate(fields):
        keep = (has_above, has_below, has_before, has_after) if f == 0 else (1.0, 1.0, 1.0, 1.0)
        ref[pl.ds(TOP - EDGE, EDGE), own_cols] = got_rows[0, f] * keep[0]
        ref[pl.ds(TOP + high, EDGE), own_cols] = got_rows[1, f] * keep[1]

        def turned(left, right):
            return jnp.concatenate([right * keep[3], gap, left * keep[2]], axis=0).T

        beside = pl.ds(wide, WIDE)
        for i in range(high // WIDE):
            at = pl.ds(i * WIDE, WIDE)
            ref[pl.ds(TOP + i * WIDE, WIDE), beside] = turned(got_cols[0, f, :, at], got_cols[1, f, :, at])
        upper = turned(got_corners[0, f], got_corners[1, f])
        ref[pl.ds(TOP - EDGE, EDGE), beside] = upper[WIDE - EDGE :] * keep[0]
        lower = turned(got_corners[2, f], got_corners[3, f])
        ref[pl.ds(TOP + high, EDGE), beside] = lower[0:EDGE] * keep[1]

    lanes = lax.broadcasted_iota(jnp.int32, (1, full), 1)
    side = jnp.where(lanes < wide, 1.0, jnp.where(lanes < wide + 64, has_after, has_before)).astype(F32)

    def laplace(ref, at, size, center):
        tall_block = jnp.concatenate(
            [ref[pl.ds(at - 8, 8), :], center, ref[pl.ds(at + size, 8), :]], axis=0
        )
        up = pltpu.roll(tall_block, 1, 0)[8 : 8 + size]
        down = pltpu.roll(tall_block, size + 15, 0)[8 : 8 + size]
        sideways = pltpu.roll(center, 1, 1) + pltpu.roll(center, full - 1, 1)
        return c[pl.ds(at, size), :] * center - (up + down + sideways)

    def inner(ref, at, size, mask):
        u[pl.ds(at, size), :] = laplace(ref, at, size, ref[pl.ds(at, size), :]) * mask

    def outer(ref, out, at, size, mask):
        here = pl.ds(at, size)
        result = w[here, :] * ref[here, :] + (smooth_weight * SCALE) * laplace(u, at, size, u[here, :])
        out[here, :] = result * mask
        return result

    def fold(x):
        total = x[:, 0:WIDE]
        for i in range(1, wide // WIDE):
            total = total + x[:, i * WIDE : (i + 1) * WIDE]
        return total.reshape(-1, 8, WIDE).sum(axis=0)

    size = 32
    zero = jnp.zeros((8, WIDE), F32)
    moments = []
    for step, (ref, out) in enumerate(((v0, v1), (v1, v2), (v2, v3))):
        inner(ref, TOP - EDGE, EDGE, side * has_above)
        inner(ref, TOP + high, EDGE, side * has_below)

        def rows_of_u(i, _, ref=ref):
            inner(ref, pl.multiple_of(TOP + i * size, 8), size, side)
            return 0

        lax.fori_loop(0, high // size, rows_of_u, 0)
        if step < 2:
            outer(ref, out, TOP - EDGE, EDGE, side * has_above)
            outer(ref, out, TOP + high, EDGE, side * has_below)

        def rows_of_v(i, sums, ref=ref, out=out, step=step):
            at = pl.multiple_of(TOP + i * size, 8)
            new = outer(ref, out, at, size, side)[:, 0:wide]
            old = ref[pl.ds(at, size), own_cols]
            terms = [old * new]
            if step == 0:
                terms.append(old * old)
            if step < 2:
                terms.append(new * new)
            return tuple(s + fold(t) for s, t in zip(sums, terms))

        sums = lax.fori_loop(0, high // size, rows_of_v, (zero,) * (3, 2, 1)[step])
        moments += [sums[1], sums[0], sums[2]] if step == 0 else list(sums)

    column = lax.broadcasted_iota(jnp.int32, (1, WIDE), 1)
    mine = jnp.zeros((1, WIDE), F32)
    for j, m in enumerate(moments):
        mine = mine + jnp.where(column == j, jnp.sum(jnp.sum(m, axis=0, keepdims=True), axis=1, keepdims=True), 0.0)
    part[...] = mine
    parts[me] = mine

    def tell(k, _):
        pr, pc = partner(row, col, rows, cols, k)
        pltpu.make_async_remote_copy(
            part, parts.at[me], sent_part, came_part, device_id=(pr, pc), device_id_type=MESH
        ).start()
        return 0

    lax.fori_loop(1, devices, tell, 0)
    others = pl.ds(1, devices - 1)
    pltpu.make_async_copy(parts.at[others], parts.at[others], came_part).wait()
    total = jnp.sum(parts[...], axis=0)
    m = [jnp.sum(jnp.where(column == j, total, 0.0), axis=1, keepdims=True) for j in range(len(moments))]
    xs, rs, growth = solve([jnp.broadcast_to(value, (1, WIDE)) for value in m])
    growth_ref[...] = growth

    def combine(i, _):
        at = pl.ds(pl.multiple_of(i * size, 8), size)
        held = pl.ds(pl.multiple_of(TOP + i * size, 8), size)

        def spread(value):
            return jnp.concatenate([jnp.broadcast_to(value, (size, WIDE))] * (wide // WIDE), axis=1)

        basis = [ref[held, own_cols] for ref in (v0, v1, v2, v3)]
        x_ref[at, :] = sum(spread(k * SCALE) * v for k, v in zip(xs, basis))
        r_ref[at, :] = sum(spread(k) * v for k, v in zip(rs, basis))
        return 0

    lax.fori_loop(0, high // size, combine, 0)
    pltpu.make_async_copy(parts.at[others], parts.at[others], sent_part).wait()


def whole(rows, cols, cell, value, weight, count, kappa, x, r, growth, wf_out, resp_out, wf, resp, *rest):
    first, second, keep = rest[:15], rest[15:-1], rest[-1]
    exchange_and_bin(rows, cols, cell, value, weight, count, wf, resp, *first)
    kept = [
        pltpu.make_async_copy(wf, wf_out, keep.at[0]),
        pltpu.make_async_copy(resp, resp_out, keep.at[1]),
    ]
    for copy in kept:
        copy.start()
    smooth(rows, cols, kappa, wf, resp, x, r, growth, *second)
    for copy in kept:
        copy.wait()


def run(rows, cols, obs_cell, obs_value, obs_weight, obs_count, kappa_field):
    devices = rows * cols
    tiles = obs_cell.shape[0]
    high, wide = kappa_field.shape
    vmem = pl.BlockSpec(memory_space=pltpu.VMEM)
    anywhere = pl.BlockSpec(memory_space=pl.ANY)
    stage = (tiles * PITCH, TILE)
    work = pltpu.VMEM((high + 2 * TOP, wide + WIDE), F32)
    dma = pltpu.SemaphoreType.DMA
    shape = jax.ShapeDtypeStruct((high, wide), F32)
    return pl.pallas_call(
        functools.partial(whole, rows, cols),
        out_shape=[shape, shape, jax.ShapeDtypeStruct((1, WIDE), F32), shape, shape],
        in_specs=[vmem] * 5,
        out_specs=[vmem] * 3 + [anywhere] * 2,
        scratch_shapes=[
            pltpu.VMEM((high, wide), F32),
            pltpu.VMEM((high, wide), F32),
            pltpu.VMEM(stage, jnp.int32),
            pltpu.VMEM(stage, F32),
            pltpu.VMEM(stage, F32),
            pltpu.VMEM((devices, tiles, TILE), jnp.int16),
            pltpu.VMEM((devices, 2 * tiles, TILE), BF),
            pltpu.VMEM((devices, tiles, TILE), jnp.int16),
            pltpu.VMEM((devices, 2 * tiles, TILE), BF),
            pltpu.VMEM((128, 128), F32),
            pltpu.VMEM((128, 128), F32),
            pltpu.VMEM((128, 128), F32),
            pltpu.VMEM((128, 128), F32),
            dma,
            dma,
            dma((devices // 8,)),
            dma((devices // 8,)),
            *[work] * 7,
            pltpu.VMEM((2, 3, EDGE, wide), F32),
            pltpu.VMEM((2, 3, EDGE, high), F32),
            pltpu.VMEM((2, 3, EDGE, wide), F32),
            pltpu.VMEM((2, 3, EDGE, high), F32),
            pltpu.VMEM((4, 3, EDGE, WIDE), F32),
            pltpu.VMEM((1, WIDE), F32),
            pltpu.VMEM((devices, 1, WIDE), F32),
            dma((8,)),
            dma((8,)),
            dma,
            dma,
            dma((2,)),
        ],
        name="bin_and_smooth",
        compiler_params=pltpu.CompilerParams(collective_id=0, has_side_effects=True),
    )(obs_cell, obs_value, obs_weight, obs_count, kappa_field)


def extended(x, sides, width):
    edges = {}
    for axis, dim in sides:
        size, length = (lax.axis_size(axis), x.shape[dim])
        up = [(i, (i + 1) % size) for i in range(size - 1)]
        last = lax.slice_in_dim(x, length - width, length, axis=dim)
        leading = lax.slice_in_dim(x, 0, width, axis=dim)
        edges[dim] = (
            lax.ppermute(last, axis, up),
            lax.ppermute(leading, axis, [(b, a) for a, b in up]),
        )
    done = []
    for _, dim in sides:
        low, high = edges[dim]
        around = [(width, width) if d in done else (0, 0) for d in range(x.ndim)]
        x = jnp.concatenate([jnp.pad(low, around), x, jnp.pad(high, around)], axis=dim)
        done.append(dim)
    return x


def one_axis_at_a_time(x, axes):
    return functools.reduce(lax.psum, axes, x)


def stencil_step(padded, kappa_field):
    center = padded[1:-1, 1:-1]
    beside = padded[2:, 1:-1] + padded[:-2, 1:-1]
    beside = beside + padded[1:-1, 2:] + padded[1:-1, :-2]
    return (4.0 + kappa_field) * center - beside


def step_by_step(weight_field, response, kappa_field):
    def operate(field):
        first = extended(field, ((ROW, 0), (COL, 1)), 1)
        inner = stencil_step(first, kappa_field)
        second = extended(inner, ((ROW, 0), (COL, 1)), 1)
        return weight_field * field + smooth_weight * stencil_step(second, kappa_field)

    solution_field = jnp.zeros_like(response)
    residual = response

    def two_products(current, image):
        return (
            one_axis_at_a_time(jnp.sum(current * current), (ROW, COL)),
            one_axis_at_a_time(jnp.sum(current * image), (ROW, COL)),
        )

    image = operate(residual)
    norm_now, curvature = two_products(residual, image)
    alpha = norm_now / curvature
    direction, along = (residual, image)
    for step in range(ITERS):
        solution_field = solution_field + alpha * direction
        residual = residual - alpha * along
        if step + 1 < ITERS:
            image = operate(residual)
            norm_next, curvature = two_products(residual, image)
            ratio = norm_next / norm_now
            alpha = norm_next / (curvature - ratio * norm_next / alpha)
            direction = residual + ratio * direction
            along = image + ratio * along
            norm_now = norm_next
    return (solution_field, residual)


def per_device(obs_cell, obs_value, obs_weight, obs_count, kappa_field):
    rows, cols = lax.axis_size(ROW), lax.axis_size(COL)
    x, r, growth, weight_field, response = run(
        rows, cols, obs_cell[0], obs_value[0], obs_weight[0], obs_count[0], kappa_field
    )
    return lax.cond(
        growth[0, 0] <= GROWTH_MAX,
        lambda x, r, *rest: (x, r),
        lambda x, r, *rest: step_by_step(*rest),
        x, r, weight_field, response, kappa_field,
    )


def solution(mesh):
    placed = (
        P((ROW, COL), None, None, None),
        P((ROW, COL), None, None, None),
        P((ROW, COL), None, None, None),
        P((ROW, COL), None, None),
        P(ROW, COL),
    )
    return jax.shard_map(
        per_device,
        mesh=mesh,
        in_specs=placed,
        out_specs=(P(ROW, COL), P(ROW, COL)),
        check_vma=False,
    )
```

```python
import functools

import jax
import jax.numpy as jnp
from jax import lax
from jax.experimental import pallas as pl
from jax.experimental.pallas import tpu as pltpu
from jax.sharding import PartitionSpec as P

TILE = 128
ITERS = 3
ROW = "row"
COL = "col"
MESH = pl.DeviceIdType.MESH
LOGICAL = pl.DeviceIdType.LOGICAL
BF = jnp.bfloat16
F32 = jnp.float32
PITCH = 136
STRIDE = 5

smooth_weight = 0.05

SCALE = 1.0 / 256.0
SHIFT = 5.0
GROWTH_MAX = 1000.0
EDGE = 8
TOP = 16
WIDE = 128


def partner(me, devices, k):
    return lax.rem(me + STRIDE * k, devices)


def each_partner(devices, act):
    for k in range(1, 8):
        act(k)

    def some(g, _):
        for k in range(8):
            act(g * 8 + k)
        return 0

    lax.fori_loop(1, devices // 8, some, 0)


def exchange_and_bin(
    rows, cols, loads, cell_ref, value_ref, weight_ref, count_ref, wf_ref, resp_ref,
    stage_c, stage_w, stage_p, send_c, send_v, got_c, got_v,
    low_s, w_s, p_s, high_t, sent_c, sent_v, came_c, came_v,
):
    devices = rows * cols
    tiles = cell_ref.shape[0]
    me = lax.axis_index(ROW) * cols + lax.axis_index(COL)
    barrier = pltpu.get_barrier_semaphore()

    def greet(k):
        pl.semaphore_signal(
            barrier, inc=1, device_id=partner(me, devices, k), device_id_type=LOGICAL
        )

    each_partner(devices, greet)
    for copy in loads:
        copy.wait()

    counts = count_ref[...].T
    slot = lax.broadcasted_iota(jnp.int32, (devices, TILE), 1)
    for t in range(tiles):
        live = slot < jnp.broadcast_to(counts[:, t : t + 1], (devices, TILE))
        cell = cell_ref[t]
        code = jnp.bitwise_and(jnp.right_shift(cell, 13 + 6), 1) * 128 + jnp.bitwise_and(cell, 127)
        code = code * 64 + jnp.bitwise_and(jnp.right_shift(cell, 13), 63)
        wide = weight_ref[t].astype(F32)
        product = (wide * value_ref[t].astype(F32)).astype(BF).astype(F32)
        stage_c[pl.ds(t * PITCH, devices), :] = code
        stage_w[pl.ds(t * PITCH, devices), :] = jnp.where(live, wide, 0.0)
        stage_p[pl.ds(t * PITCH, devices), :] = jnp.where(live, product, 0.0)

    def gather(g, _):
        for j in range(8):
            k = g * 8 + j
            rows_at = pl.ds(partner(me, devices, k), tiles, stride=PITCH)
            send_c[k] = stage_c[rows_at, :].astype(jnp.int16)
            send_v[k, 0:16, :] = stage_w[rows_at, :].astype(BF)
            send_v[k, 16:32, :] = stage_p[rows_at, :].astype(BF)
        return 0

    lax.fori_loop(0, devices // 8, gather, 0)
    pl.semaphore_wait(barrier, devices - 1)

    def send(k):
        to = partner(me, devices, k)
        pltpu.make_async_remote_copy(
            send_c.at[k], got_c.at[k], sent_c, came_c.at[k // 8], device_id=to, device_id_type=LOGICAL
        ).start()
        pltpu.make_async_remote_copy(
            send_v.at[k], got_v.at[k], sent_v, came_v.at[k // 8], device_id=to, device_id_type=LOGICAL
        ).start()

    each_partner(devices, send)
    got_c[0] = send_c[0]
    got_v[0] = send_v[0]
    wf_ref[...] = jnp.zeros_like(wf_ref)
    resp_ref[...] = jnp.zeros_like(resp_ref)

    lanes = lax.broadcasted_iota(jnp.int32, (16, 128), 1).astype(F32)
    high_ids = [lanes.astype(BF), (lanes + 128.0).astype(BF)]
    subs = lax.broadcasted_iota(jnp.int32, (16, 128), 0).astype(F32)
    low_ids = [(subs + 16.0 * g).astype(BF) for g in range(4)]
    one, zero = jnp.ones((16, 128), BF), jnp.zeros((16, 128), BF)
    across = wf_ref.shape[1] // TILE

    def bin_group(g):
        code = got_c[pl.ds(g * 8, 8)].reshape(128, 128).astype(jnp.int32)
        low_s[...] = jnp.bitwise_and(code, 63).astype(F32)
        high_t[...] = jnp.right_shift(code, 6).astype(F32).T
        for s in range(8):
            w_s[pl.ds(s * 16, 16), :] = got_v[g * 8 + s, 0:16, :].astype(F32)
            p_s[pl.ds(s * 16, 16), :] = got_v[g * 8 + s, 16:32, :].astype(F32)
        for t in range(tiles):
            total = None
            for pair in range(4):
                left, right = [], []
                for s in (2 * pair, 2 * pair + 1):
                    r = s * 16 + t
                    low, w, p = (
                        jnp.broadcast_to(ref[pl.ds(r, 1), :], (16, 128)).astype(BF)
                        for ref in (low_s, w_s, p_s)
                    )
                    hits = [low == ids for ids in low_ids]
                    left.append(
                        jnp.concatenate(
                            [jnp.where(h, w, zero) for h in hits]
                            + [jnp.where(h, p, zero) for h in hits],
                            axis=0,
                        )
                    )
                    high = jnp.broadcast_to(high_t[:, r : r + 1], (128, 128)).astype(BF)
                    for v in range(8):
                        part = high[16 * v : 16 * v + 16]
                        right.append(
                            jnp.concatenate([jnp.where(part == ids, one, zero) for ids in high_ids], axis=1)
                        )
                piece = jnp.dot(
                    jnp.concatenate(left, axis=1),
                    jnp.concatenate(right, axis=0),
                    preferred_element_type=F32,
                )
                total = piece if total is None else total + piece
            for ref, at in ((wf_ref, 0), (resp_ref, 64)):
                for half in range(2):
                    where = (
                        pl.ds((t // across) * TILE + half * 64, 64),
                        pl.ds((t % across) * TILE, TILE),
                    )
                    ref[where] = ref[where] + total[at : at + 64, half * 128 : half * 128 + 128]

    def arrived(first, size, g):
        there = pl.ds(first, size)
        pltpu.make_async_copy(got_c.at[there], got_c.at[there], came_c.at[g]).wait()
        pltpu.make_async_copy(got_v.at[there], got_v.at[there], came_v.at[g]).wait()

    def step(g, _):
        @pl.when(g == 0)
        def _():
            arrived(1, 7, 0)

        @pl.when(g > 0)
        def _():
            arrived(g * 8, 8, g)

        bin_group(g)
        return 0

    lax.fori_loop(0, devices // 8, step, 0)
    out = pl.ds(1, devices - 1)
    pltpu.make_async_copy(send_c.at[out], send_c.at[out], sent_c).wait()
    pltpu.make_async_copy(send_v.at[out], send_v.at[out], sent_v).wait()


def solve(m):
    shift = SCALE * SHIFT

    def at(p, i):
        return p[i] if 0 <= i < len(p) else None

    def plus(a, b):
        return b if a is None else a if b is None else a + b

    def dot(a, b):
        total, size = None, None
        for i, x in enumerate(a):
            for j, y in enumerate(b):
                term = x * y * m[i + j]
                total, size = plus(total, term), plus(size, jnp.abs(term))
        return total, size / jnp.abs(total)

    def times_a(p):
        out = []
        for i in range(len(p) + 1):
            scaled = None if at(p, i) is None else shift * p[i]
            out.append(plus(scaled, at(p, i - 1)))
        return out

    def axpy(a, b, c):
        return [
            plus(at(a, i), None if at(b, i) is None else c * b[i]) for i in range(max(len(a), len(b)))
        ]

    one = jnp.ones_like(m[0])
    x, r, p, rr, growth = [], [one], [one], m[0], one
    for step in range(ITERS):
        ap = times_a(p)
        pap, grown = dot(p, ap)
        growth = jnp.where(grown <= growth, growth, grown)
        alpha = rr / pap
        x, r = axpy(x, p, alpha), axpy(r, ap, -alpha)
        if step + 1 < ITERS:
            new, grown = dot(r, r)
            growth = jnp.where(grown <= growth, growth, grown)
            p, rr = axpy(r, p, new / rr), new
    return x, r, growth


def smooth(
    rows, cols, while_waiting, kappa_ref, wf_ref, resp_ref, x_ref, r_ref, growth_ref,
    v0, v1, v2, v3, u, w, c, send_rows, send_cols, got_rows, got_cols, got_corners,
    part, parts, sent_edge, came_edge, sent_part, came_part,
):
    devices = rows * cols
    high, wide = kappa_ref.shape
    row, col = lax.axis_index(ROW), lax.axis_index(COL)
    me = row * cols + col
    above, below = (row + rows - 1) % rows, (row + 1) % rows
    before, after = (col + cols - 1) % cols, (col + 1) % cols
    has_above = jnp.where(row > 0, 1.0, 0.0).astype(F32)
    has_below = jnp.where(row < rows - 1, 1.0, 0.0).astype(F32)
    has_before = jnp.where(col > 0, 1.0, 0.0).astype(F32)
    has_after = jnp.where(col < cols - 1, 1.0, 0.0).astype(F32)
    tall = high + 2 * TOP
    full = wide + WIDE
    own_rows, own_cols = pl.ds(TOP, high), pl.ds(0, wide)

    fields = (v0, w, c)
    for ref in (v0, w, c, u, v1, v2):
        ref[pl.ds(0, TOP), :] = jnp.zeros((TOP, full), F32)
        ref[pl.ds(TOP + high, TOP), :] = jnp.zeros((TOP, full), F32)
    v0[own_rows, own_cols] = resp_ref[...]
    w[own_rows, own_cols] = (wf_ref[...] - SHIFT) * SCALE
    c[own_rows, own_cols] = kappa_ref[...] + 4.0
    lane = lax.broadcasted_iota(jnp.int32, (WIDE, WIDE), 1)
    for f, ref in enumerate(fields):
        send_rows[0, f] = ref[pl.ds(TOP, EDGE), own_cols]
        send_rows[1, f] = ref[pl.ds(TOP + high - EDGE, EDGE), own_cols]
        for i in range(high // WIDE):
            block = pl.ds(TOP + i * WIDE, WIDE)
            left = ref[block, pl.ds(0, WIDE)]
            right = ref[block, pl.ds(wide - WIDE, WIDE)]
            turned = jnp.where(lane < 64, left, right).T
            send_cols[0, f, :, pl.ds(i * WIDE, WIDE)] = turned[0:EDGE]
            send_cols[1, f, :, pl.ds(i * WIDE, WIDE)] = turned[WIDE - EDGE :]

    def copies():
        first, last = pl.ds(0, WIDE), pl.ds(high - WIDE, WIDE)
        plan = [
            (send_rows.at[0], got_rows.at[1], above, col),
            (send_rows.at[1], got_rows.at[0], below, col),
            (send_cols.at[0], got_cols.at[1], row, before),
            (send_cols.at[1], got_cols.at[0], row, after),
            (send_cols.at[0, :, :, first], got_corners.at[3], above, before),
            (send_cols.at[0, :, :, last], got_corners.at[1], below, before),
            (send_cols.at[1, :, :, first], got_corners.at[2], above, after),
            (send_cols.at[1, :, :, last], got_corners.at[0], below, after),
        ]
        return [
            pltpu.make_async_remote_copy(
                source, target, sent_edge.at[i], came_edge.at[i], device_id=(pr, pc), device_id_type=MESH
            )
            for i, (source, target, pr, pc) in enumerate(plan)
        ]

    edges = copies()
    for copy in edges:
        copy.start()
    for copy in edges:
        copy.wait()
    gap = jnp.zeros((WIDE - 2 * EDGE, WIDE), F32)
    for f, ref in enumerate(fields):
        keep = (has_above, has_below, has_before, has_after) if f == 0 else (1.0, 1.0, 1.0, 1.0)
        ref[pl.ds(TOP - EDGE, EDGE), own_cols] = got_rows[0, f] * keep[0]
        ref[pl.ds(TOP + high, EDGE), own_cols] = got_rows[1, f] * keep[1]

        def turned(left, right):
            return jnp.concatenate([right * keep[3], gap, left * keep[2]], axis=0).T

        beside = pl.ds(wide, WIDE)
        for i in range(high // WIDE):
            at = pl.ds(i * WIDE, WIDE)
            ref[pl.ds(TOP + i * WIDE, WIDE), beside] = turned(got_cols[0, f, :, at], got_cols[1, f, :, at])
        upper = turned(got_corners[0, f], got_corners[1, f])
        ref[pl.ds(TOP - EDGE, EDGE), beside] = upper[WIDE - EDGE :] * keep[0]
        lower = turned(got_corners[2, f], got_corners[3, f])
        ref[pl.ds(TOP + high, EDGE), beside] = lower[0:EDGE] * keep[1]

    lanes = lax.broadcasted_iota(jnp.int32, (1, full), 1)
    side = jnp.where(lanes < wide, 1.0, jnp.where(lanes < wide + 64, has_after, has_before)).astype(F32)

    def laplace(ref, at, size, center):
        tall_block = jnp.concatenate(
            [ref[pl.ds(at - 8, 8), :], center, ref[pl.ds(at + size, 8), :]], axis=0
        )
        up = pltpu.roll(tall_block, 1, 0)[8 : 8 + size]
        down = pltpu.roll(tall_block, size + 15, 0)[8 : 8 + size]
        sideways = pltpu.roll(center, 1, 1) + pltpu.roll(center, full - 1, 1)
        return c[pl.ds(at, size), :] * center - (up + down + sideways)

    def inner(ref, at, size, mask):
        u[pl.ds(at, size), :] = laplace(ref, at, size, ref[pl.ds(at, size), :]) * mask

    def outer(ref, out, at, size, mask):
        here = pl.ds(at, size)
        result = w[here, :] * ref[here, :] + (smooth_weight * SCALE) * laplace(u, at, size, u[here, :])
        out[here, :] = result * mask
        return result

    def fold(x):
        total = x[:, 0:WIDE]
        for i in range(1, wide // WIDE):
            total = total + x[:, i * WIDE : (i + 1) * WIDE]
        return total.reshape(-1, 8, WIDE).sum(axis=0)

    size = 32
    zero = jnp.zeros((8, WIDE), F32)
    moments = []
    for step, (ref, out) in enumerate(((v0, v1), (v1, v2), (v2, v3))):
        inner(ref, TOP - EDGE, EDGE, side * has_above)
        inner(ref, TOP + high, EDGE, side * has_below)

        def rows_of_u(i, _, ref=ref):
            inner(ref, pl.multiple_of(TOP + i * size, 8), size, side)
            return 0

        lax.fori_loop(0, high // size, rows_of_u, 0)
        if step < 2:
            outer(ref, out, TOP - EDGE, EDGE, side * has_above)
            outer(ref, out, TOP + high, EDGE, side * has_below)

        def rows_of_v(i, sums, ref=ref, out=out, step=step):
            at = pl.multiple_of(TOP + i * size, 8)
            new = outer(ref, out, at, size, side)[:, 0:wide]
            old = ref[pl.ds(at, size), own_cols]
            terms = [old * new]
            if step == 0:
                terms.append(old * old)
            if step < 2:
                terms.append(new * new)
            return tuple(s + fold(t) for s, t in zip(sums, terms))

        sums = lax.fori_loop(0, high // size, rows_of_v, (zero,) * (3, 2, 1)[step])
        moments += [sums[1], sums[0], sums[2]] if step == 0 else list(sums)

    column = lax.broadcasted_iota(jnp.int32, (1, WIDE), 1)
    mine = jnp.zeros((1, WIDE), F32)
    for j, m in enumerate(moments):
        mine = mine + jnp.where(column == j, jnp.sum(jnp.sum(m, axis=0, keepdims=True), axis=1, keepdims=True), 0.0)
    part[...] = mine
    parts[me] = mine

    def tell(k):
        to = partner(me, devices, k)
        pltpu.make_async_remote_copy(
            part, parts.at[me], sent_part, came_part, device_id=to, device_id_type=LOGICAL
        ).start()

    each_partner(devices, tell)
    while_waiting()
    others = pl.ds(1, devices - 1)
    pltpu.make_async_copy(parts.at[others], parts.at[others], came_part).wait()
    total = jnp.sum(parts[...], axis=0)
    m = [jnp.sum(jnp.where(column == j, total, 0.0), axis=1, keepdims=True) for j in range(len(moments))]
    xs, rs, growth = solve([jnp.broadcast_to(value, (1, WIDE)) for value in m])
    growth_ref[...] = growth

    def combine(i, _):
        at = pl.ds(pl.multiple_of(i * size, 8), size)
        held = pl.ds(pl.multiple_of(TOP + i * size, 8), size)

        def spread(value):
            return jnp.concatenate([jnp.broadcast_to(value, (size, WIDE))] * (wide // WIDE), axis=1)

        basis = [ref[held, own_cols] for ref in (v0, v1, v2, v3)]
        x_ref[at, :] = sum(spread(k * SCALE) * v for k, v in zip(xs, basis))
        r_ref[at, :] = sum(spread(k) * v for k, v in zip(rs, basis))
        return 0

    lax.fori_loop(0, high // size, combine, 0)
    pltpu.make_async_copy(parts.at[others], parts.at[others], sent_part).wait()


def whole(rows, cols, *refs):
    inputs, (x, r, growth, *kept), inside, (wf, resp) = refs[:5], refs[5:10], refs[10:15], refs[15:17]
    first, second, moved = refs[17:32], refs[32:-1], refs[-1]
    loads = [pltpu.make_async_copy(a, b, moved.at[i]) for i, (a, b) in enumerate(zip(inputs, inside))]
    for copy in loads:
        copy.start()
    stores = [pltpu.make_async_copy(a, b, moved.at[5 + i]) for i, (a, b) in enumerate(zip((wf, resp), kept))]
    exchange_and_bin(rows, cols, loads[:4], *inside[:4], wf, resp, *first)
    loads[4].wait()

    def while_waiting():
        for copy in stores:
            copy.start()

    smooth(rows, cols, while_waiting, inside[4], wf, resp, x, r, growth, *second)
    for copy in stores:
        copy.wait()


def hand_over(*refs):
    copies = [pltpu.make_async_copy(refs[i], refs[2 + i], refs[4].at[i]) for i in range(2)]
    for copy in copies:
        copy.start()
    for copy in copies:
        copy.wait()


def deliver(x, r):
    return pl.pallas_call(
        hand_over,
        out_shape=[jax.ShapeDtypeStruct(a.shape, a.dtype) for a in (x, r)],
        in_specs=[pl.BlockSpec(memory_space=pl.ANY)] * 2,
        out_specs=[pl.BlockSpec(memory_space=pltpu.HBM)] * 2,
        scratch_shapes=[pltpu.SemaphoreType.DMA((2,))],
        name="deliver",
    )(x, r)


def run(rows, cols, obs_cell, obs_value, obs_weight, obs_count, kappa_field):
    devices = rows * cols
    tiles = obs_cell.shape[0]
    high, wide = kappa_field.shape
    arguments = (obs_cell, obs_value, obs_weight, obs_count, kappa_field)
    vmem = pl.BlockSpec(memory_space=pltpu.VMEM)
    hbm = pl.BlockSpec(memory_space=pltpu.HBM)
    stage = (tiles * PITCH, TILE)
    work = pltpu.VMEM((high + 2 * TOP, wide + WIDE), F32)
    dma = pltpu.SemaphoreType.DMA
    shape = jax.ShapeDtypeStruct((high, wide), F32)
    return pl.pallas_call(
        functools.partial(whole, rows, cols),
        out_shape=[pltpu.VMEM((high, wide), F32), pltpu.VMEM((high, wide), F32), pltpu.VMEM((1, WIDE), F32), shape, shape],
        in_specs=[hbm] * 5,
        out_specs=[vmem] * 3 + [hbm] * 2,
        scratch_shapes=[
            *[pltpu.VMEM(a.shape, a.dtype) for a in arguments],
            pltpu.VMEM((high, wide), F32),
            pltpu.VMEM((high, wide), F32),
            pltpu.VMEM(stage, jnp.int32),
            pltpu.VMEM(stage, F32),
            pltpu.VMEM(stage, F32),
            pltpu.VMEM((devices, tiles, TILE), jnp.int16),
            pltpu.VMEM((devices, 2 * tiles, TILE), BF),
            pltpu.VMEM((devices, tiles, TILE), jnp.int16),
            pltpu.VMEM((devices, 2 * tiles, TILE), BF),
            pltpu.VMEM((128, 128), F32),
            pltpu.VMEM((128, 128), F32),
            pltpu.VMEM((128, 128), F32),
            pltpu.VMEM((128, 128), F32),
            dma,
            dma,
            dma((devices // 8,)),
            dma((devices // 8,)),
            *[work] * 7,
            pltpu.VMEM((2, 3, EDGE, wide), F32),
            pltpu.VMEM((2, 3, EDGE, high), F32),
            pltpu.VMEM((2, 3, EDGE, wide), F32),
            pltpu.VMEM((2, 3, EDGE, high), F32),
            pltpu.VMEM((4, 3, EDGE, WIDE), F32),
            pltpu.VMEM((1, WIDE), F32),
            pltpu.VMEM((devices, 1, WIDE), F32),
            dma((8,)),
            dma((8,)),
            dma,
            dma,
            dma((7,)),
        ],
        name="bin_and_smooth",
        compiler_params=pltpu.CompilerParams(collective_id=0, has_side_effects=True),
    )(*arguments)


def extended(x, sides, width):
    edges = {}
    for axis, dim in sides:
        size, length = (lax.axis_size(axis), x.shape[dim])
        up = [(i, (i + 1) % size) for i in range(size - 1)]
        last = lax.slice_in_dim(x, length - width, length, axis=dim)
        leading = lax.slice_in_dim(x, 0, width, axis=dim)
        edges[dim] = (
            lax.ppermute(last, axis, up),
            lax.ppermute(leading, axis, [(b, a) for a, b in up]),
        )
    done = []
    for _, dim in sides:
        low, high = edges[dim]
        around = [(width, width) if d in done else (0, 0) for d in range(x.ndim)]
        x = jnp.concatenate([jnp.pad(low, around), x, jnp.pad(high, around)], axis=dim)
        done.append(dim)
    return x


def one_axis_at_a_time(x, axes):
    return functools.reduce(lax.psum, axes, x)


def stencil_step(padded, kappa_field):
    center = padded[1:-1, 1:-1]
    beside = padded[2:, 1:-1] + padded[:-2, 1:-1]
    beside = beside + padded[1:-1, 2:] + padded[1:-1, :-2]
    return (4.0 + kappa_field) * center - beside


def step_by_step(weight_field, response, kappa_field):
    def operate(field):
        first = extended(field, ((ROW, 0), (COL, 1)), 1)
        inner = stencil_step(first, kappa_field)
        second = extended(inner, ((ROW, 0), (COL, 1)), 1)
        return weight_field * field + smooth_weight * stencil_step(second, kappa_field)

    solution_field = jnp.zeros_like(response)
    residual = response

    def two_products(current, image):
        return (
            one_axis_at_a_time(jnp.sum(current * current), (ROW, COL)),
            one_axis_at_a_time(jnp.sum(current * image), (ROW, COL)),
        )

    image = operate(residual)
    norm_now, curvature = two_products(residual, image)
    alpha = norm_now / curvature
    direction, along = (residual, image)
    for step in range(ITERS):
        solution_field = solution_field + alpha * direction
        residual = residual - alpha * along
        if step + 1 < ITERS:
            image = operate(residual)
            norm_next, curvature = two_products(residual, image)
            ratio = norm_next / norm_now
            alpha = norm_next / (curvature - ratio * norm_next / alpha)
            direction = residual + ratio * direction
            along = image + ratio * along
            norm_now = norm_next
    return (solution_field, residual)


def per_device(obs_cell, obs_value, obs_weight, obs_count, kappa_field):
    rows, cols = lax.axis_size(ROW), lax.axis_size(COL)
    x, r, growth, weight_field, response = run(
        rows, cols, obs_cell[0], obs_value[0], obs_weight[0], obs_count[0], kappa_field
    )
    return lax.cond(
        growth[0, 0] <= GROWTH_MAX,
        lambda x, r, *rest: tuple(deliver(x, r)),
        lambda x, r, *rest: step_by_step(*rest),
        x, r, weight_field, response, kappa_field,
    )


def solution(mesh):
    placed = (
        P((ROW, COL), None, None, None),
        P((ROW, COL), None, None, None),
        P((ROW, COL), None, None, None),
        P((ROW, COL), None, None),
        P(ROW, COL),
    )
    return jax.shard_map(
        per_device,
        mesh=mesh,
        in_specs=placed,
        out_specs=(P(ROW, COL), P(ROW, COL)),
        check_vma=False,
    )
```

```python
import functools

import jax
import jax.numpy as jnp
from jax import lax
from jax.experimental import pallas as pl
from jax.experimental.pallas import tpu as pltpu
from jax.sharding import PartitionSpec as P

TILE = 128
ITERS = 3
ROW = "row"
COL = "col"
MESH = pl.DeviceIdType.MESH
LOGICAL = pl.DeviceIdType.LOGICAL
BF = jnp.bfloat16
F32 = jnp.float32
PITCH = 136
STRIDE = 5
GROUP = 16

smooth_weight = 0.05

SCALE = 1.0 / 256.0
SHIFT = 5.0
GROWTH_MAX = 1000.0
EDGE = 8
RIM = 6
WIDE = 128


def partner(me, devices, k):
    return lax.rem(me + STRIDE * k, devices)


def each_partner(devices, act):
    for k in range(1, 8):
        act(k)

    def some(g, _):
        for k in range(8):
            act(g * 8 + k)
        return 0

    lax.fori_loop(1, devices // 8, some, 0)


def exchange_and_bin(
    rows, cols, loads, ready, sent_out, cell_ref, value_ref, weight_ref, count_ref, wf_ref, resp_ref,
    stage_c, stage_w, stage_p, send_c, send_v, got_c, got_v,
    low_s, w_s, p_s, high_s, sent_c, sent_v, came_c, came_v,
):
    devices = rows * cols
    tiles = cell_ref.shape[0]
    me = lax.axis_index(ROW) * cols + lax.axis_index(COL)
    barrier = pltpu.get_barrier_semaphore()

    def greet(k):
        pl.semaphore_signal(
            barrier, inc=1, device_id=partner(me, devices, k), device_id_type=LOGICAL
        )

    each_partner(devices, greet)
    for copy in loads:
        copy.wait()

    counts = count_ref[...].T
    slot = lax.broadcasted_iota(jnp.int32, (devices, TILE), 1)
    for t in range(tiles):
        live = slot < jnp.broadcast_to(counts[:, t : t + 1], (devices, TILE))
        cell = cell_ref[t]
        code = jnp.bitwise_and(jnp.right_shift(cell, 13 + 6), 1) * 128 + jnp.bitwise_and(cell, 127)
        code = code * 64 + jnp.bitwise_and(jnp.right_shift(cell, 13), 63)
        wide = weight_ref[t].astype(F32)
        product = (wide * value_ref[t].astype(F32)).astype(BF).astype(F32)
        stage_c[pl.ds(t * PITCH, devices), :] = code
        stage_w[pl.ds(t * PITCH, devices), :] = jnp.where(live, wide, 0.0)
        stage_p[pl.ds(t * PITCH, devices), :] = jnp.where(live, product, 0.0)

    def gather(g, _):
        for j in range(8):
            k = g * 8 + j
            rows_at = pl.ds(partner(me, devices, k), tiles, stride=PITCH)
            send_c[k] = stage_c[rows_at, :].astype(jnp.int16)
            send_v[k, 0:16, :] = stage_w[rows_at, :].astype(BF)
            send_v[k, 16:32, :] = stage_p[rows_at, :].astype(BF)
        return 0

    lax.fori_loop(0, devices // 8, gather, 0)
    ready()
    pl.semaphore_wait(barrier, devices - 1)

    def send(k):
        to = partner(me, devices, k)
        pltpu.make_async_remote_copy(
            send_c.at[k], got_c.at[k], sent_c, came_c.at[k // GROUP], device_id=to, device_id_type=LOGICAL
        ).start()
        pltpu.make_async_remote_copy(
            send_v.at[k], got_v.at[k], sent_v, came_v.at[k // GROUP], device_id=to, device_id_type=LOGICAL
        ).start()

    each_partner(devices, send)
    sent_out()
    got_c[0] = send_c[0]
    got_v[0] = send_v[0]
    wf_ref[...] = jnp.zeros_like(wf_ref)
    resp_ref[...] = jnp.zeros_like(resp_ref)

    lanes = lax.broadcasted_iota(jnp.int32, (16, 128), 1).astype(F32)
    high_ids = [lanes.astype(BF), (lanes + 128.0).astype(BF)]
    subs = lax.broadcasted_iota(jnp.int32, (16, 128), 0).astype(F32)
    low_ids = [(subs + 16.0 * g).astype(BF) for g in range(4)]
    one, zero = jnp.ones((16, 128), BF), jnp.zeros((16, 128), BF)
    across = wf_ref.shape[1] // TILE

    def bin_group(g):
        code = got_c[pl.ds(g * GROUP, GROUP)].reshape(GROUP * tiles, 128).astype(jnp.int32)
        low_s[...] = jnp.bitwise_and(code, 63).astype(F32)
        high_s[...] = jnp.right_shift(code, 6).astype(F32)
        for s in range(GROUP):
            w_s[pl.ds(s * 16, 16), :] = got_v[g * GROUP + s, 0:16, :].astype(F32)
            p_s[pl.ds(s * 16, 16), :] = got_v[g * GROUP + s, 16:32, :].astype(F32)
        for t in range(tiles):
            total = None
            for pair in range(GROUP // 2):
                left, right = [], []
                for s in (2 * pair, 2 * pair + 1):
                    r = s * 16 + t
                    low, high, w, p = (
                        jnp.broadcast_to(ref[pl.ds(r, 1), :], (16, 128)).astype(BF)
                        for ref in (low_s, high_s, w_s, p_s)
                    )
                    hits = [low == ids for ids in low_ids]
                    left.append(
                        jnp.concatenate(
                            [jnp.where(h, w, zero) for h in hits]
                            + [jnp.where(h, p, zero) for h in hits],
                            axis=0,
                        )
                    )
                    turned = jnp.concatenate([high] * 8, axis=0).T
                    for v in range(8):
                        part = turned[16 * v : 16 * v + 16]
                        right.append(
                            jnp.concatenate([jnp.where(part == ids, one, zero) for ids in high_ids], axis=1)
                        )
                piece = jnp.dot(
                    jnp.concatenate(left, axis=1),
                    jnp.concatenate(right, axis=0),
                    preferred_element_type=F32,
                )
                total = piece if total is None else total + piece
            for ref, at in ((wf_ref, 0), (resp_ref, 64)):
                for half in range(2):
                    where = (
                        pl.ds((t // across) * TILE + half * 64, 64),
                        pl.ds((t % across) * TILE, TILE),
                    )
                    ref[where] = ref[where] + total[at : at + 64, half * 128 : half * 128 + 128]

    def arrived(first, size, g):
        there = pl.ds(first, size)
        pltpu.make_async_copy(got_c.at[there], got_c.at[there], came_c.at[g]).wait()
        pltpu.make_async_copy(got_v.at[there], got_v.at[there], came_v.at[g]).wait()

    def step(g, _):
        @pl.when(g == 0)
        def _():
            arrived(1, GROUP - 1, 0)

        @pl.when(g > 0)
        def _():
            arrived(g * GROUP, GROUP, g)

        bin_group(g)
        return 0

    lax.fori_loop(0, devices // GROUP, step, 0)
    out = pl.ds(1, devices - 1)
    pltpu.make_async_copy(send_c.at[out], send_c.at[out], sent_c).wait()
    pltpu.make_async_copy(send_v.at[out], send_v.at[out], sent_v).wait()


def solve(m):
    shift = SCALE * SHIFT

    def at(p, i):
        return p[i] if 0 <= i < len(p) else None

    def plus(a, b):
        return b if a is None else a if b is None else a + b

    def dot(a, b):
        total, size = None, None
        for i, x in enumerate(a):
            for j, y in enumerate(b):
                term = x * y * m[i + j]
                total, size = plus(total, term), plus(size, jnp.abs(term))
        return total, size / jnp.abs(total)

    def times_a(p):
        out = []
        for i in range(len(p) + 1):
            scaled = None if at(p, i) is None else shift * p[i]
            out.append(plus(scaled, at(p, i - 1)))
        return out

    def axpy(a, b, c):
        return [
            plus(at(a, i), None if at(b, i) is None else c * b[i]) for i in range(max(len(a), len(b)))
        ]

    one = jnp.ones_like(m[0])
    x, r, p, rr, growth = [], [one], [one], m[0], one
    for step in range(ITERS):
        ap = times_a(p)
        pap, grown = dot(p, ap)
        growth = jnp.where(grown <= growth, growth, grown)
        alpha = rr / pap
        x, r = axpy(x, p, alpha), axpy(r, ap, -alpha)
        if step + 1 < ITERS:
            new, grown = dot(r, r)
            growth = jnp.where(grown <= growth, growth, grown)
            p, rr = axpy(r, p, new / rr), new
    return x, r, growth


class Edges:
    def __init__(self, rows, cols, rows_out, cols_out, rows_in, cols_in, corners, sent, came):
        row, col = lax.axis_index(ROW), lax.axis_index(COL)
        above, below = lax.rem(row + rows - 1, rows), lax.rem(row + 1, rows)
        before, after = lax.rem(col + cols - 1, cols), lax.rem(col + 1, cols)
        self.rows_out, self.cols_out = rows_out, cols_out
        self.rows_in, self.cols_in, self.corners = rows_in, cols_in, corners
        last = cols_out.shape[2] - 1
        plan = [
            (rows_out.at[0], rows_in.at[1], above, col),
            (rows_out.at[1], rows_in.at[0], below, col),
            (cols_out.at[0], cols_in.at[1], row, before),
            (cols_out.at[1], cols_in.at[0], row, after),
            (cols_out.at[0, :, 0], corners.at[3], above, before),
            (cols_out.at[0, :, last], corners.at[1], below, before),
            (cols_out.at[1, :, 0], corners.at[2], above, after),
            (cols_out.at[1, :, last], corners.at[0], below, after),
        ]
        self.copies = [
            pltpu.make_async_remote_copy(
                source, target, sent.at[i], came.at[i], device_id=(pr, pc), device_id_type=MESH
            )
            for i, (source, target, pr, pc) in enumerate(plan)
        ]

    def start(self):
        for copy in self.copies:
            copy.start()

    def wait(self):
        for copy in self.copies:
            copy.wait()


def lay_out(ref, field):
    high, wide = field.shape
    strip = high // 8
    for s in range(8):
        for j in range(wide // WIDE):
            ref[j, pl.ds(RIM * 8 + s, strip, stride=8), :] = field[s * strip : (s + 1) * strip, j * WIDE : (j + 1) * WIDE]


def group(i, n=1):
    return pl.ds(i * 8, n * 8)


def pack_edges(ref, f, edges, top, bottom):
    lane = lax.broadcasted_iota(jnp.int32, (8, WIDE), 1)
    tiles = ref.shape[0] - 1
    edges.rows_out[0, f] = top
    edges.rows_out[1, f] = bottom
    for q in range(edges.cols_out.shape[2]):
        left, right = jnp.zeros((8, WIDE), F32), jnp.zeros((8, WIDE), F32)
        for n in range(16):
            slot = (lane >= 8 * n) & (lane < 8 * n + 8)
            at = group(RIM + 16 * q + n)
            left = jnp.where(slot, pltpu.roll(ref[0, at, :], 8 * n, 1), left)
            right = jnp.where(slot, pltpu.roll(ref[tiles - 1, at, :], (8 * n + 8) % WIDE, 1), right)
        edges.cols_out[0, f, q] = left
        edges.cols_out[1, f, q] = right


def fill_edges(ref, f, edges, keep):
    lane = lax.broadcasted_iota(jnp.int32, (8, WIDE), 1)
    sub = lax.broadcasted_iota(jnp.int32, (8, WIDE), 0)
    tiles = ref.shape[0] - 1
    strip = ref.shape[1] // 8 - 2 * RIM
    above, below, before, after = keep

    def beside(left, right, n):
        left = pltpu.roll(left, (120 - 8 * n) % WIDE, 1)
        right = pltpu.roll(right, (WIDE - 8 * n) % WIDE, 1)
        return jnp.where(lane < 8, right * after, jnp.where(lane >= 120, left * before, 0.0))

    for i in range(strip):
        q, n = i // 16, i % 16
        ref[tiles, group(RIM + i), :] = beside(edges.cols_in[0, f, q], edges.cols_in[1, f, q], n)
    for j in range(tiles + 1):
        for i in range(RIM):
            if j < tiles:
                up = edges.rows_in[0, f, EDGE - RIM + i : EDGE - RIM + i + 1, j * WIDE : (j + 1) * WIDE]
                down = edges.rows_in[1, f, i : i + 1, j * WIDE : (j + 1) * WIDE]
                up, down = (jnp.broadcast_to(x, (8, WIDE)) for x in (up, down))
            else:
                up = beside(edges.corners[0, f], edges.corners[1, f], 16 - RIM + i)
                down = beside(edges.corners[2, f], edges.corners[3, f], i)
                up, down = pltpu.roll(up, 1, 0), pltpu.roll(down, 7, 0)
            inside = pltpu.roll(ref[j, group(strip + i), :], 1, 0)
            ref[j, group(i), :] = jnp.where(sub == 0, up * above, inside)
            inside = pltpu.roll(ref[j, group(RIM + i), :], 7, 0)
            ref[j, group(RIM + strip + i), :] = jnp.where(sub == 7, down * below, inside)


def smooth(
    rows, cols, while_waiting, early, late, wf_ref, resp_ref, x_ref, r_ref, growth_ref,
    v0, v1, v2, v3, u, w, c, y1, y2, y3, part, parts, sent_part, came_part,
):
    devices = rows * cols
    high, wide = x_ref.shape
    tiles, strip = wide // WIDE, high // 8
    row, col = lax.axis_index(ROW), lax.axis_index(COL)
    me = row * cols + col
    keep = tuple(
        jnp.where(there, 1.0, 0.0).astype(F32)
        for there in (row > 0, row < rows - 1, col > 0, col < cols - 1)
    )

    lay_out(v0, resp_ref[...])
    lay_out(w, (wf_ref[...] - SHIFT) * SCALE)
    first, last = slice(0, EDGE), slice(high - EDGE, high)
    pack_edges(v0, 0, late, resp_ref[first, :], resp_ref[last, :])
    pack_edges(w, 1, late, (wf_ref[first, :] - SHIFT) * SCALE, (wf_ref[last, :] - SHIFT) * SCALE)
    late.start()
    early.wait()
    fill_edges(c, 0, early, (1.0,) * 4)
    late.wait()
    fill_edges(v0, 0, late, keep)
    fill_edges(w, 1, late, (1.0,) * 4)

    lane = lax.broadcasted_iota(jnp.int32, (8, WIDE), 1)
    sub = lax.broadcasted_iota(jnp.int32, (8, WIDE), 0)
    side = jnp.where(lane < 64, keep[3], keep[2])
    upper = jnp.where(sub == 0, keep[0], 1.0)
    lower = jnp.where(sub == 7, keep[1], 1.0)

    def laplace(ref, i, n):
        size = n * 8
        lanes = lax.broadcasted_iota(jnp.int32, (size, WIDE), 1)
        tall = [ref[j, group(i - 1, n + 2), :] for j in range(tiles + 1)]
        here = [x[8 : 8 + size] for x in tall]
        later = [pltpu.roll(x, 1, 1) for x in here]
        sooner = [pltpu.roll(x, WIDE - 1, 1) for x in here]
        out = []
        for j in range(tiles + 1):
            left = jnp.where(lanes == 0, later[j - 1], later[j])
            right = jnp.where(lanes == WIDE - 1, sooner[(j + 1) % (tiles + 1)], sooner[j])
            beside = (tall[j][0:size] + tall[j][16 : 16 + size]) + (left + right)
            out.append(c[j, group(i, n), :] * here[j] - beside)
        return out, here

    def masked(x, n, j, edge):
        if edge is not None:
            x = x * jnp.concatenate([edge] * n, axis=0)
        if j == tiles:
            x = x * jnp.concatenate([side] * n, axis=0)
        return x

    def inner(ref, i, n, edge=None):
        news, olds = laplace(ref, i, n)
        news = [masked(x, n, j, edge) for j, x in enumerate(news)]
        for j, x in enumerate(news):
            u[j, group(i, n), :] = x
        return news[:tiles], olds[:tiles]

    def outer(ref, out, i, n, edge=None):
        news, olds = [], []
        for j, x in enumerate(laplace(u, i, n)[0]):
            old = ref[j, group(i, n), :]
            new = masked(w[j, group(i, n), :] * old + (smooth_weight * SCALE) * x, n, j, edge)
            out[j, group(i, n), :] = new
            news.append(new)
            olds.append(old)
        return news[:tiles], olds[:tiles]

    def fold(pairs, n):
        total = None
        for a, b in pairs:
            product = a * b
            for i in range(n):
                piece = product[i * 8 : i * 8 + 8]
                total = piece if total is None else total + piece
        return total

    n = 16
    zero = jnp.zeros((8, WIDE), F32)
    moments = []
    for step, (ref, out) in enumerate(((v0, v1), (v1, v2), (v2, v3))):
        rim = RIM - 1 - 2 * step
        inner(ref, RIM - rim, rim, upper)
        inner(ref, RIM + strip, rim, lower)

        def rows_of_u(k, sums, ref=ref, step=step):
            news, olds = inner(ref, RIM + k * n, n)
            if step < 2:
                return sums
            weighted = [w[j, group(RIM + k * n, n), :] * x for j, x in enumerate(olds)]
            return sums[0] + fold(zip(weighted, olds), n), sums[1] + fold(zip(news, news), n)

        sums = lax.fori_loop(0, strip // n, rows_of_u, (zero,) * (0, 0, 2)[step])
        if step == 2:
            moments.append(sums[0] + (smooth_weight * SCALE) * sums[1])
            break
        outer(ref, out, RIM - rim + 1, rim - 1, upper)
        outer(ref, out, RIM + strip, rim - 1, lower)

        def rows_of_v(k, sums, ref=ref, out=out, step=step):
            news, olds = outer(ref, out, RIM + k * n, n)
            terms = [fold(zip(olds, news), n), fold(zip(news, news), n)]
            if step == 0:
                terms.append(fold(zip(olds, olds), n))
            return tuple(s + t for s, t in zip(sums, terms))

        sums = lax.fori_loop(0, strip // n, rows_of_v, (zero,) * (3, 2)[step])
        moments += [sums[2], sums[0], sums[1]] if step == 0 else list(sums)

    column = lax.broadcasted_iota(jnp.int32, (1, WIDE), 1)
    mine = jnp.zeros((1, WIDE), F32)
    for j, m in enumerate(moments):
        mine = mine + jnp.where(column == j, jnp.sum(jnp.sum(m, axis=0, keepdims=True), axis=1, keepdims=True), 0.0)
    part[...] = mine
    parts[me] = mine

    def tell(k):
        to = partner(me, devices, k)
        pltpu.make_async_remote_copy(
            part, parts.at[me], sent_part, came_part, device_id=to, device_id_type=LOGICAL
        ).start()

    each_partner(devices, tell)
    while_waiting()

    def rows_of_last(k, _):
        outer(v2, v3, RIM + k * n, n)
        return 0

    lax.fori_loop(0, strip // n, rows_of_last, 0)

    def straighten(s, _):
        for j in range(tiles):
            place = (pl.ds(s * strip, strip), pl.ds(j * WIDE, WIDE))
            for ref, flat in ((v1, y1), (v2, y2), (v3, y3)):
                flat[place] = ref[j, pl.ds(RIM * 8 + s, strip, stride=8), :]
        return 0

    lax.fori_loop(0, 8, straighten, 0)
    others = pl.ds(1, devices - 1)
    pltpu.make_async_copy(parts.at[others], parts.at[others], came_part).wait()
    total = jnp.sum(parts[...], axis=0)
    m = [jnp.sum(jnp.where(column == j, total, 0.0), axis=1, keepdims=True) for j in range(len(moments))]
    xs, rs, growth = solve([jnp.broadcast_to(value, (1, WIDE)) for value in m])
    growth_ref[...] = growth

    def spread(value):
        return jnp.concatenate([jnp.broadcast_to(value, (32, WIDE))] * tiles, axis=1)

    def combine(k, _):
        at = pl.ds(k * 32, 32)
        basis = [ref[at, :] for ref in (resp_ref, y1, y2, y3)]
        x_ref[at, :] = sum(spread(a * SCALE) * v for a, v in zip(xs, basis))
        r_ref[at, :] = sum(spread(a) * v for a, v in zip(rs, basis))
        return 0

    lax.fori_loop(0, high // 32, combine, 0)
    pltpu.make_async_copy(parts.at[others], parts.at[others], sent_part).wait()


def whole(rows, cols, *refs):
    inputs, (x, r, growth, *kept), inside, (wf, resp) = refs[:5], refs[5:10], refs[10:15], refs[15:17]
    first, second, moved = refs[17:32], refs[32:46], refs[60]
    early, late = Edges(rows, cols, *refs[46:53]), Edges(rows, cols, *refs[53:60])
    kappa, c = inside[4], second[6]
    loads = [pltpu.make_async_copy(a, b, moved.at[i]) for i, (a, b) in enumerate(zip(inputs, inside))]
    for copy in loads:
        copy.start()
    stores = [pltpu.make_async_copy(a, b, moved.at[5 + i]) for i, (a, b) in enumerate(zip((wf, resp), kept))]

    def ready():
        loads[4].wait()
        lay_out(c, kappa[...] + 4.0)
        high = kappa.shape[0]
        pack_edges(c, 0, early, kappa[0:EDGE, :] + 4.0, kappa[high - EDGE : high, :] + 4.0)

    exchange_and_bin(rows, cols, loads[:4], ready, early.start, *inside[:4], wf, resp, *first)

    def while_waiting():
        for copy in stores:
            copy.start()

    smooth(rows, cols, while_waiting, early, late, wf, resp, x, r, growth, *second)
    for copy in stores:
        copy.wait()


def hand_over(*refs):
    copies = [pltpu.make_async_copy(refs[i], refs[2 + i], refs[4].at[i]) for i in range(2)]
    for copy in copies:
        copy.start()
    for copy in copies:
        copy.wait()


def deliver(x, r):
    return pl.pallas_call(
        hand_over,
        out_shape=[jax.ShapeDtypeStruct(a.shape, a.dtype) for a in (x, r)],
        in_specs=[pl.BlockSpec(memory_space=pl.ANY)] * 2,
        out_specs=[pl.BlockSpec(memory_space=pltpu.HBM)] * 2,
        scratch_shapes=[pltpu.SemaphoreType.DMA((2,))],
        name="deliver",
    )(x, r)


def run(rows, cols, obs_cell, obs_value, obs_weight, obs_count, kappa_field):
    devices = rows * cols
    tiles = obs_cell.shape[0]
    high, wide = kappa_field.shape
    arguments = (obs_cell, obs_value, obs_weight, obs_count, kappa_field)
    vmem = pl.BlockSpec(memory_space=pltpu.VMEM)
    hbm = pl.BlockSpec(memory_space=pltpu.HBM)
    stage = (tiles * PITCH, TILE)
    work = pltpu.VMEM((wide // WIDE + 1, (high // 8 + 2 * RIM) * 8, WIDE), F32)

    def edges(count):
        ends = pltpu.VMEM((2, count, EDGE, wide), F32)
        sides = pltpu.VMEM((2, count, high // WIDE, 8, WIDE), F32)
        return [ends, sides, ends, sides, pltpu.VMEM((4, count, 8, WIDE), F32), dma((8,)), dma((8,))]

    dma = pltpu.SemaphoreType.DMA
    shape = jax.ShapeDtypeStruct((high, wide), F32)
    return pl.pallas_call(
        functools.partial(whole, rows, cols),
        out_shape=[pltpu.VMEM((high, wide), F32), pltpu.VMEM((high, wide), F32), pltpu.VMEM((1, WIDE), F32), shape, shape],
        in_specs=[hbm] * 5,
        out_specs=[vmem] * 3 + [hbm] * 2,
        scratch_shapes=[
            *[pltpu.VMEM(a.shape, a.dtype) for a in arguments],
            pltpu.VMEM((high, wide), F32),
            pltpu.VMEM((high, wide), F32),
            pltpu.VMEM(stage, jnp.int32),
            pltpu.VMEM(stage, F32),
            pltpu.VMEM(stage, F32),
            pltpu.VMEM((devices, tiles, TILE), jnp.int16),
            pltpu.VMEM((devices, 2 * tiles, TILE), BF),
            pltpu.VMEM((devices, tiles, TILE), jnp.int16),
            pltpu.VMEM((devices, 2 * tiles, TILE), BF),
            *[pltpu.VMEM((GROUP * tiles, TILE), F32)] * 4,
            dma,
            dma,
            dma((devices // GROUP,)),
            dma((devices // GROUP,)),
            *[work] * 7,
            *[pltpu.VMEM((high, wide), F32)] * 3,
            pltpu.VMEM((1, WIDE), F32),
            pltpu.VMEM((devices, 1, WIDE), F32),
            dma,
            dma,
            *edges(1),
            *edges(2),
            dma((7,)),
        ],
        name="bin_and_smooth",
        compiler_params=pltpu.CompilerParams(collective_id=0, has_side_effects=True),
    )(*arguments)


def extended(x, sides, width):
    edges = {}
    for axis, dim in sides:
        size, length = (lax.axis_size(axis), x.shape[dim])
        up = [(i, (i + 1) % size) for i in range(size - 1)]
        last = lax.slice_in_dim(x, length - width, length, axis=dim)
        leading = lax.slice_in_dim(x, 0, width, axis=dim)
        edges[dim] = (
            lax.ppermute(last, axis, up),
            lax.ppermute(leading, axis, [(b, a) for a, b in up]),
        )
    done = []
    for _, dim in sides:
        low, high = edges[dim]
        around = [(width, width) if d in done else (0, 0) for d in range(x.ndim)]
        x = jnp.concatenate([jnp.pad(low, around), x, jnp.pad(high, around)], axis=dim)
        done.append(dim)
    return x


def one_axis_at_a_time(x, axes):
    return functools.reduce(lax.psum, axes, x)


def stencil_step(padded, kappa_field):
    center = padded[1:-1, 1:-1]
    beside = padded[2:, 1:-1] + padded[:-2, 1:-1]
    beside = beside + padded[1:-1, 2:] + padded[1:-1, :-2]
    return (4.0 + kappa_field) * center - beside


def step_by_step(weight_field, response, kappa_field):
    def operate(field):
        first = extended(field, ((ROW, 0), (COL, 1)), 1)
        inner = stencil_step(first, kappa_field)
        second = extended(inner, ((ROW, 0), (COL, 1)), 1)
        return weight_field * field + smooth_weight * stencil_step(second, kappa_field)

    solution_field = jnp.zeros_like(response)
    residual = response

    def two_products(current, image):
        return (
            one_axis_at_a_time(jnp.sum(current * current), (ROW, COL)),
            one_axis_at_a_time(jnp.sum(current * image), (ROW, COL)),
        )

    image = operate(residual)
    norm_now, curvature = two_products(residual, image)
    alpha = norm_now / curvature
    direction, along = (residual, image)
    for step in range(ITERS):
        solution_field = solution_field + alpha * direction
        residual = residual - alpha * along
        if step + 1 < ITERS:
            image = operate(residual)
            norm_next, curvature = two_products(residual, image)
            ratio = norm_next / norm_now
            alpha = norm_next / (curvature - ratio * norm_next / alpha)
            direction = residual + ratio * direction
            along = image + ratio * along
            norm_now = norm_next
    return (solution_field, residual)


def per_device(obs_cell, obs_value, obs_weight, obs_count, kappa_field):
    rows, cols = lax.axis_size(ROW), lax.axis_size(COL)
    x, r, growth, weight_field, response = run(
        rows, cols, obs_cell[0], obs_value[0], obs_weight[0], obs_count[0], kappa_field
    )
    return lax.cond(
        growth[0, 0] <= GROWTH_MAX,
        lambda x, r, *rest: tuple(deliver(x, r)),
        lambda x, r, *rest: step_by_step(*rest),
        x, r, weight_field, response, kappa_field,
    )


def solution(mesh):
    placed = (
        P((ROW, COL), None, None, None),
        P((ROW, COL), None, None, None),
        P((ROW, COL), None, None, None),
        P((ROW, COL), None, None),
        P(ROW, COL),
    )
    return jax.shard_map(
        per_device,
        mesh=mesh,
        in_specs=placed,
        out_specs=(P(ROW, COL), P(ROW, COL)),
        check_vma=False,
    )
```

```python
import functools

import jax
import jax.numpy as jnp
from jax import lax
from jax.experimental import pallas as pl
from jax.experimental.pallas import tpu as pltpu
from jax.sharding import PartitionSpec as P

TILE = 128
ITERS = 3
ROW = "row"
COL = "col"
MESH = pl.DeviceIdType.MESH
LOGICAL = pl.DeviceIdType.LOGICAL
BF = jnp.bfloat16
F32 = jnp.float32
PITCH = 136
STRIDE = 5
GROUP = 16

smooth_weight = 0.05

SCALE = 1.0 / 256.0
SHIFT = 5.0
GROWTH_MAX = 1000.0
EDGE = 8
RIM = 6
WIDE = 128


def partner(me, devices, k):
    return lax.rem(me + STRIDE * k, devices)


def each_partner(devices, act):
    for k in range(1, 8):
        act(k)

    def some(g, _):
        for k in range(8):
            act(g * 8 + k)
        return 0

    lax.fori_loop(1, devices // 8, some, 0)


def exchange_and_bin(
    rows, cols, loads, ready, sent_out, cell_ref, value_ref, weight_ref, count_ref, wf_ref, resp_ref,
    stage_c, stage_w, stage_p, send_c, send_v, got_c, got_v,
    low_s, w_s, p_s, high_s, sent_c, sent_v, came_c, came_v,
):
    devices = rows * cols
    tiles = cell_ref.shape[0]
    me = lax.axis_index(ROW) * cols + lax.axis_index(COL)
    barrier = pltpu.get_barrier_semaphore()

    def greet(k):
        pl.semaphore_signal(
            barrier, inc=1, device_id=partner(me, devices, k), device_id_type=LOGICAL
        )

    each_partner(devices, greet)
    for copy in loads:
        copy.wait()

    counts = count_ref[...].T
    slot = lax.broadcasted_iota(jnp.int32, (devices, TILE), 1)
    for t in range(tiles):
        live = slot < jnp.broadcast_to(counts[:, t : t + 1], (devices, TILE))
        cell = cell_ref[t]
        code = jnp.bitwise_and(jnp.right_shift(cell, 13 + 6), 1) * 128 + jnp.bitwise_and(cell, 127)
        code = code * 64 + jnp.bitwise_and(jnp.right_shift(cell, 13), 63)
        wide = weight_ref[t].astype(F32)
        product = (wide * value_ref[t].astype(F32)).astype(BF).astype(F32)
        stage_c[pl.ds(t * PITCH, devices), :] = code
        stage_w[pl.ds(t * PITCH, devices), :] = jnp.where(live, wide, 0.0)
        stage_p[pl.ds(t * PITCH, devices), :] = jnp.where(live, product, 0.0)

    def gather(g, _):
        for j in range(8):
            k = g * 8 + j
            rows_at = pl.ds(partner(me, devices, k), tiles, stride=PITCH)
            send_c[k] = stage_c[rows_at, :].astype(jnp.int16)
            send_v[k, 0:16, :] = stage_w[rows_at, :].astype(BF)
            send_v[k, 16:32, :] = stage_p[rows_at, :].astype(BF)
        return 0

    lax.fori_loop(0, devices // 8, gather, 0)
    ready()
    pl.semaphore_wait(barrier, devices - 1)

    def send(k):
        to = partner(me, devices, k)
        pltpu.make_async_remote_copy(
            send_c.at[k], got_c.at[k], sent_c, came_c.at[k // GROUP], device_id=to, device_id_type=LOGICAL
        ).start()
        pltpu.make_async_remote_copy(
            send_v.at[k], got_v.at[k], sent_v, came_v.at[k // GROUP], device_id=to, device_id_type=LOGICAL
        ).start()

    each_partner(devices, send)
    sent_out()
    got_c[0] = send_c[0]
    got_v[0] = send_v[0]
    wf_ref[...] = jnp.zeros_like(wf_ref)
    resp_ref[...] = jnp.zeros_like(resp_ref)

    lanes = lax.broadcasted_iota(jnp.int32, (16, 128), 1).astype(F32)
    high_ids = [lanes.astype(BF), (lanes + 128.0).astype(BF)]
    subs = lax.broadcasted_iota(jnp.int32, (16, 128), 0).astype(F32)
    low_ids = [(subs + 16.0 * g).astype(BF) for g in range(4)]
    one, zero = jnp.ones((16, 128), BF), jnp.zeros((16, 128), BF)
    across = wf_ref.shape[1] // TILE

    def bin_group(g):
        code = got_c[pl.ds(g * GROUP, GROUP)].reshape(GROUP * tiles, 128).astype(jnp.int32)
        low_s[...] = jnp.bitwise_and(code, 63).astype(F32)
        high_s[...] = jnp.right_shift(code, 6).astype(F32)
        for s in range(GROUP):
            w_s[pl.ds(s * 16, 16), :] = got_v[g * GROUP + s, 0:16, :].astype(F32)
            p_s[pl.ds(s * 16, 16), :] = got_v[g * GROUP + s, 16:32, :].astype(F32)
        for t in range(tiles):
            total = None
            for pair in range(GROUP // 2):
                left, right = [], []
                for s in (2 * pair, 2 * pair + 1):
                    r = s * 16 + t
                    low, high, w, p = (
                        jnp.broadcast_to(ref[pl.ds(r, 1), :], (16, 128)).astype(BF)
                        for ref in (low_s, high_s, w_s, p_s)
                    )
                    hits = [low == ids for ids in low_ids]
                    left.append(
                        jnp.concatenate(
                            [jnp.where(h, w, zero) for h in hits]
                            + [jnp.where(h, p, zero) for h in hits],
                            axis=0,
                        )
                    )
                    turned = jnp.concatenate([high] * 8, axis=0).T
                    for v in range(8):
                        part = turned[16 * v : 16 * v + 16]
                        right.append(
                            jnp.concatenate([jnp.where(part == ids, one, zero) for ids in high_ids], axis=1)
                        )
                piece = jnp.dot(
                    jnp.concatenate(left, axis=1),
                    jnp.concatenate(right, axis=0),
                    preferred_element_type=F32,
                )
                total = piece if total is None else total + piece
            for ref, at in ((wf_ref, 0), (resp_ref, 64)):
                for half in range(2):
                    where = (
                        pl.ds((t // across) * TILE + half * 64, 64),
                        pl.ds((t % across) * TILE, TILE),
                    )
                    ref[where] = ref[where] + total[at : at + 64, half * 128 : half * 128 + 128]

    def arrived(first, size, g):
        there = pl.ds(first, size)
        pltpu.make_async_copy(got_c.at[there], got_c.at[there], came_c.at[g]).wait()
        pltpu.make_async_copy(got_v.at[there], got_v.at[there], came_v.at[g]).wait()

    def step(g, _):
        @pl.when(g == 0)
        def _():
            arrived(1, GROUP - 1, 0)

        @pl.when(g > 0)
        def _():
            arrived(g * GROUP, GROUP, g)

        bin_group(g)
        return 0

    lax.fori_loop(0, devices // GROUP, step, 0)
    out = pl.ds(1, devices - 1)
    pltpu.make_async_copy(send_c.at[out], send_c.at[out], sent_c).wait()
    pltpu.make_async_copy(send_v.at[out], send_v.at[out], sent_v).wait()


def solve(m):
    shift = SCALE * SHIFT

    def at(p, i):
        return p[i] if 0 <= i < len(p) else None

    def plus(a, b):
        return b if a is None else a if b is None else a + b

    def dot(a, b):
        total, size = None, None
        for i, x in enumerate(a):
            for j, y in enumerate(b):
                term = x * y * m[i + j]
                total, size = plus(total, term), plus(size, jnp.abs(term))
        return total, size / jnp.abs(total)

    def times_a(p):
        out = []
        for i in range(len(p) + 1):
            scaled = None if at(p, i) is None else shift * p[i]
            out.append(plus(scaled, at(p, i - 1)))
        return out

    def axpy(a, b, c):
        return [
            plus(at(a, i), None if at(b, i) is None else c * b[i]) for i in range(max(len(a), len(b)))
        ]

    one = jnp.ones_like(m[0])
    x, r, p, rr, growth = [], [one], [one], m[0], one
    for step in range(ITERS):
        ap = times_a(p)
        pap, grown = dot(p, ap)
        growth = jnp.where(grown <= growth, growth, grown)
        alpha = rr / pap
        x, r = axpy(x, p, alpha), axpy(r, ap, -alpha)
        if step + 1 < ITERS:
            new, grown = dot(r, r)
            growth = jnp.where(grown <= growth, growth, grown)
            p, rr = axpy(r, p, new / rr), new
    return x, r, growth


class Edges:
    def __init__(self, rows, cols, rows_out, cols_out, rows_in, cols_in, corners, sent, came):
        row, col = lax.axis_index(ROW), lax.axis_index(COL)
        above, below = lax.rem(row + rows - 1, rows), lax.rem(row + 1, rows)
        before, after = lax.rem(col + cols - 1, cols), lax.rem(col + 1, cols)
        self.rows_out, self.cols_out = rows_out, cols_out
        self.rows_in, self.cols_in, self.corners = rows_in, cols_in, corners
        last = cols_out.shape[2] - 1
        plan = [
            (rows_out.at[0], rows_in.at[1], above, col),
            (rows_out.at[1], rows_in.at[0], below, col),
            (cols_out.at[0], cols_in.at[1], row, before),
            (cols_out.at[1], cols_in.at[0], row, after),
            (cols_out.at[0, :, 0], corners.at[3], above, before),
            (cols_out.at[0, :, last], corners.at[1], below, before),
            (cols_out.at[1, :, 0], corners.at[2], above, after),
            (cols_out.at[1, :, last], corners.at[0], below, after),
        ]
        self.copies = [
            pltpu.make_async_remote_copy(
                source, target, sent.at[i], came.at[i], device_id=(pr, pc), device_id_type=MESH
            )
            for i, (source, target, pr, pc) in enumerate(plan)
        ]

    def start(self):
        for copy in self.copies:
            copy.start()

    def wait(self):
        for copy in self.copies:
            copy.wait()


def lay_out(ref, field):
    high, wide = field.shape
    strip = high // 8
    for s in range(8):
        for j in range(wide // WIDE):
            ref[j, pl.ds(RIM * 8 + s, strip, stride=8), :] = field[s * strip : (s + 1) * strip, j * WIDE : (j + 1) * WIDE]


def group(i, n=1):
    return pl.ds(i * 8, n * 8)


def pack_edges(ref, f, edges, top, bottom):
    lane = lax.broadcasted_iota(jnp.int32, (8, WIDE), 1)
    tiles = ref.shape[0] - 1
    edges.rows_out[0, f] = top
    edges.rows_out[1, f] = bottom
    for q in range(edges.cols_out.shape[2]):
        left, right = jnp.zeros((8, WIDE), F32), jnp.zeros((8, WIDE), F32)
        for n in range(16):
            slot = (lane >= 8 * n) & (lane < 8 * n + 8)
            at = group(RIM + 16 * q + n)
            left = jnp.where(slot, pltpu.roll(ref[0, at, :], 8 * n, 1), left)
            right = jnp.where(slot, pltpu.roll(ref[tiles - 1, at, :], (8 * n + 8) % WIDE, 1), right)
        edges.cols_out[0, f, q] = left
        edges.cols_out[1, f, q] = right


def fill_edges(ref, f, edges, keep):
    lane = lax.broadcasted_iota(jnp.int32, (8, WIDE), 1)
    sub = lax.broadcasted_iota(jnp.int32, (8, WIDE), 0)
    tiles = ref.shape[0] - 1
    strip = ref.shape[1] // 8 - 2 * RIM
    above, below, before, after = keep

    def beside(left, right, n):
        left = pltpu.roll(left, (120 - 8 * n) % WIDE, 1)
        right = pltpu.roll(right, (WIDE - 8 * n) % WIDE, 1)
        return jnp.where(lane < 8, right * after, jnp.where(lane >= 120, left * before, 0.0))

    for i in range(strip):
        q, n = i // 16, i % 16
        ref[tiles, group(RIM + i), :] = beside(edges.cols_in[0, f, q], edges.cols_in[1, f, q], n)
    for j in range(tiles + 1):
        for i in range(RIM):
            if j < tiles:
                up = edges.rows_in[0, f, EDGE - RIM + i : EDGE - RIM + i + 1, j * WIDE : (j + 1) * WIDE]
                down = edges.rows_in[1, f, i : i + 1, j * WIDE : (j + 1) * WIDE]
                up, down = (jnp.broadcast_to(x, (8, WIDE)) for x in (up, down))
            else:
                up = beside(edges.corners[0, f], edges.corners[1, f], 16 - RIM + i)
                down = beside(edges.corners[2, f], edges.corners[3, f], i)
                up, down = pltpu.roll(up, 1, 0), pltpu.roll(down, 7, 0)
            inside = pltpu.roll(ref[j, group(strip + i), :], 1, 0)
            ref[j, group(i), :] = jnp.where(sub == 0, up * above, inside)
            inside = pltpu.roll(ref[j, group(RIM + i), :], 7, 0)
            ref[j, group(RIM + strip + i), :] = jnp.where(sub == 7, down * below, inside)


def smooth(
    rows, cols, while_waiting, early, middle, late, wf_ref, resp_ref, x_ref, r_ref, growth_ref,
    v0, v1, v2, v3, u, w, c, y1, y2, y3, part, parts, sent_part, came_part,
):
    devices = rows * cols
    high, wide = x_ref.shape
    tiles, strip = wide // WIDE, high // 8
    row, col = lax.axis_index(ROW), lax.axis_index(COL)
    me = row * cols + col
    keep = tuple(
        jnp.where(there, 1.0, 0.0).astype(F32)
        for there in (row > 0, row < rows - 1, col > 0, col < cols - 1)
    )

    first, last = slice(0, EDGE), slice(high - EDGE, high)
    lay_out(v0, resp_ref[...])
    pack_edges(v0, 0, middle, resp_ref[first, :], resp_ref[last, :])
    middle.start()
    lay_out(w, (wf_ref[...] - SHIFT) * SCALE)
    pack_edges(w, 0, late, (wf_ref[first, :] - SHIFT) * SCALE, (wf_ref[last, :] - SHIFT) * SCALE)
    late.start()
    early.wait()
    fill_edges(c, 0, early, (1.0,) * 4)
    middle.wait()
    fill_edges(v0, 0, middle, keep)

    lane = lax.broadcasted_iota(jnp.int32, (8, WIDE), 1)
    sub = lax.broadcasted_iota(jnp.int32, (8, WIDE), 0)
    side = jnp.where(lane < 64, keep[3], keep[2])
    upper = jnp.where(sub == 0, keep[0], 1.0)
    lower = jnp.where(sub == 7, keep[1], 1.0)

    def laplace(ref, i, n):
        size = n * 8
        lanes = lax.broadcasted_iota(jnp.int32, (size, WIDE), 1)
        tall = [ref[j, group(i - 1, n + 2), :] for j in range(tiles + 1)]
        here = [x[8 : 8 + size] for x in tall]
        later = [pltpu.roll(x, 1, 1) for x in here]
        sooner = [pltpu.roll(x, WIDE - 1, 1) for x in here]
        out = []
        for j in range(tiles + 1):
            left = jnp.where(lanes == 0, later[j - 1], later[j])
            right = jnp.where(lanes == WIDE - 1, sooner[(j + 1) % (tiles + 1)], sooner[j])
            beside = (tall[j][0:size] + tall[j][16 : 16 + size]) + (left + right)
            out.append(c[j, group(i, n), :] * here[j] - beside)
        return out, here

    def masked(x, n, j, edge):
        if edge is not None:
            x = x * jnp.concatenate([edge] * n, axis=0)
        if j == tiles:
            x = x * jnp.concatenate([side] * n, axis=0)
        return x

    def inner(ref, i, n, edge=None):
        news, olds = laplace(ref, i, n)
        news = [masked(x, n, j, edge) for j, x in enumerate(news)]
        for j, x in enumerate(news):
            u[j, group(i, n), :] = x
        return news[:tiles], olds[:tiles]

    def outer(ref, out, i, n, edge=None):
        news, olds = [], []
        for j, x in enumerate(laplace(u, i, n)[0]):
            old = ref[j, group(i, n), :]
            new = masked(w[j, group(i, n), :] * old + (smooth_weight * SCALE) * x, n, j, edge)
            out[j, group(i, n), :] = new
            news.append(new)
            olds.append(old)
        return news[:tiles], olds[:tiles]

    def fold(pairs, n):
        total = None
        for a, b in pairs:
            product = a * b
            for i in range(n):
                piece = product[i * 8 : i * 8 + 8]
                total = piece if total is None else total + piece
        return total

    n = 32
    zero = jnp.zeros((8, WIDE), F32)
    moments = []
    for step, (ref, out) in enumerate(((v0, v1), (v1, v2), (v2, v3))):
        rim = RIM - 1 - 2 * step
        inner(ref, RIM - rim, rim, upper)
        inner(ref, RIM + strip, rim, lower)

        def rows_of_u(k, sums, ref=ref, step=step):
            news, olds = inner(ref, RIM + k * n, n)
            if step < 2:
                return sums
            weighted = [w[j, group(RIM + k * n, n), :] * x for j, x in enumerate(olds)]
            return sums[0] + fold(zip(weighted, olds), n), sums[1] + fold(zip(news, news), n)

        sums = lax.fori_loop(0, strip // n, rows_of_u, (zero,) * (0, 0, 2)[step])
        if step == 2:
            moments.append(sums[0] + (smooth_weight * SCALE) * sums[1])
            break
        if step == 0:
            late.wait()
            fill_edges(w, 0, late, (1.0,) * 4)
        outer(ref, out, RIM - rim + 1, rim - 1, upper)
        outer(ref, out, RIM + strip, rim - 1, lower)

        def rows_of_v(k, sums, ref=ref, out=out, step=step):
            news, olds = outer(ref, out, RIM + k * n, n)
            terms = [fold(zip(olds, news), n), fold(zip(news, news), n)]
            if step == 0:
                terms.append(fold(zip(olds, olds), n))
            return tuple(s + t for s, t in zip(sums, terms))

        sums = lax.fori_loop(0, strip // n, rows_of_v, (zero,) * (3, 2)[step])
        moments += [sums[2], sums[0], sums[1]] if step == 0 else list(sums)

    column = lax.broadcasted_iota(jnp.int32, (1, WIDE), 1)
    mine = jnp.zeros((1, WIDE), F32)
    for j, m in enumerate(moments):
        mine = mine + jnp.where(column == j, jnp.sum(jnp.sum(m, axis=0, keepdims=True), axis=1, keepdims=True), 0.0)
    part[...] = mine
    parts[me] = mine

    def tell(k):
        to = partner(me, devices, k)
        pltpu.make_async_remote_copy(
            part, parts.at[me], sent_part, came_part, device_id=to, device_id_type=LOGICAL
        ).start()

    each_partner(devices, tell)
    while_waiting()

    def rows_of_last(k, _):
        outer(v2, v3, RIM + k * n, n)
        return 0

    lax.fori_loop(0, strip // n, rows_of_last, 0)

    def straighten(s, _):
        for j in range(tiles):
            place = (pl.ds(s * strip, strip), pl.ds(j * WIDE, WIDE))
            for ref, flat in ((v1, y1), (v2, y2), (v3, y3)):
                flat[place] = ref[j, pl.ds(RIM * 8 + s, strip, stride=8), :]
        return 0

    lax.fori_loop(0, 8, straighten, 0)
    others = pl.ds(1, devices - 1)
    pltpu.make_async_copy(parts.at[others], parts.at[others], came_part).wait()
    total = jnp.sum(parts[...], axis=0)
    m = [jnp.sum(jnp.where(column == j, total, 0.0), axis=1, keepdims=True) for j in range(len(moments))]
    xs, rs, growth = solve([jnp.broadcast_to(value, (1, WIDE)) for value in m])
    growth_ref[...] = growth

    def spread(value):
        return jnp.concatenate([jnp.broadcast_to(value, (32, WIDE))] * tiles, axis=1)

    def combine(k, _):
        at = pl.ds(k * 32, 32)
        basis = [ref[at, :] for ref in (resp_ref, y1, y2, y3)]
        x_ref[at, :] = sum(spread(a * SCALE) * v for a, v in zip(xs, basis))
        r_ref[at, :] = sum(spread(a) * v for a, v in zip(rs, basis))
        return 0

    lax.fori_loop(0, high // 32, combine, 0)
    pltpu.make_async_copy(parts.at[others], parts.at[others], sent_part).wait()


def whole(rows, cols, *refs):
    inputs, (x, r, growth, *kept), inside, (wf, resp) = refs[:5], refs[5:10], refs[10:15], refs[15:17]
    first, second, moved = refs[17:32], refs[32:46], refs[67]
    early, middle, late = (Edges(rows, cols, *refs[i : i + 7]) for i in (46, 53, 60))
    kappa, c = inside[4], second[6]
    loads = [pltpu.make_async_copy(a, b, moved.at[i]) for i, (a, b) in enumerate(zip(inputs, inside))]
    for copy in loads:
        copy.start()
    stores = [pltpu.make_async_copy(a, b, moved.at[5 + i]) for i, (a, b) in enumerate(zip((wf, resp), kept))]

    def ready():
        loads[4].wait()
        lay_out(c, kappa[...] + 4.0)
        high = kappa.shape[0]
        pack_edges(c, 0, early, kappa[0:EDGE, :] + 4.0, kappa[high - EDGE : high, :] + 4.0)

    exchange_and_bin(rows, cols, loads[:4], ready, early.start, *inside[:4], wf, resp, *first)

    def while_waiting():
        for copy in stores:
            copy.start()

    smooth(rows, cols, while_waiting, early, middle, late, wf, resp, x, r, growth, *second)
    for copy in stores:
        copy.wait()


def hand_over(*refs):
    copies = [pltpu.make_async_copy(refs[i], refs[2 + i], refs[4].at[i]) for i in range(2)]
    for copy in copies:
        copy.start()
    for copy in copies:
        copy.wait()


def deliver(x, r):
    return pl.pallas_call(
        hand_over,
        out_shape=[jax.ShapeDtypeStruct(a.shape, a.dtype) for a in (x, r)],
        in_specs=[pl.BlockSpec(memory_space=pl.ANY)] * 2,
        out_specs=[pl.BlockSpec(memory_space=pltpu.HBM)] * 2,
        scratch_shapes=[pltpu.SemaphoreType.DMA((2,))],
        name="deliver",
    )(x, r)


def run(rows, cols, obs_cell, obs_value, obs_weight, obs_count, kappa_field):
    devices = rows * cols
    tiles = obs_cell.shape[0]
    high, wide = kappa_field.shape
    arguments = (obs_cell, obs_value, obs_weight, obs_count, kappa_field)
    vmem = pl.BlockSpec(memory_space=pltpu.VMEM)
    hbm = pl.BlockSpec(memory_space=pltpu.HBM)
    stage = (tiles * PITCH, TILE)
    work = pltpu.VMEM((wide // WIDE + 1, (high // 8 + 2 * RIM) * 8, WIDE), F32)

    def edges(count):
        ends = pltpu.VMEM((2, count, EDGE, wide), F32)
        sides = pltpu.VMEM((2, count, high // WIDE, 8, WIDE), F32)
        return [ends, sides, ends, sides, pltpu.VMEM((4, count, 8, WIDE), F32), dma((8,)), dma((8,))]

    dma = pltpu.SemaphoreType.DMA
    shape = jax.ShapeDtypeStruct((high, wide), F32)
    return pl.pallas_call(
        functools.partial(whole, rows, cols),
        out_shape=[pltpu.VMEM((high, wide), F32), pltpu.VMEM((high, wide), F32), pltpu.VMEM((1, WIDE), F32), shape, shape],
        in_specs=[hbm] * 5,
        out_specs=[vmem] * 3 + [hbm] * 2,
        scratch_shapes=[
            *[pltpu.VMEM(a.shape, a.dtype) for a in arguments],
            pltpu.VMEM((high, wide), F32),
            pltpu.VMEM((high, wide), F32),
            pltpu.VMEM(stage, jnp.int32),
            pltpu.VMEM(stage, F32),
            pltpu.VMEM(stage, F32),
            pltpu.VMEM((devices, tiles, TILE), jnp.int16),
            pltpu.VMEM((devices, 2 * tiles, TILE), BF),
            pltpu.VMEM((devices, tiles, TILE), jnp.int16),
            pltpu.VMEM((devices, 2 * tiles, TILE), BF),
            *[pltpu.VMEM((GROUP * tiles, TILE), F32)] * 4,
            dma,
            dma,
            dma((devices // GROUP,)),
            dma((devices // GROUP,)),
            *[work] * 7,
            *[pltpu.VMEM((high, wide), F32)] * 3,
            pltpu.VMEM((1, WIDE), F32),
            pltpu.VMEM((devices, 1, WIDE), F32),
            dma,
            dma,
            *edges(1),
            *edges(1),
            *edges(1),
            dma((7,)),
        ],
        name="bin_and_smooth",
        compiler_params=pltpu.CompilerParams(collective_id=0, has_side_effects=True),
    )(*arguments)


def extended(x, sides, width):
    edges = {}
    for axis, dim in sides:
        size, length = (lax.axis_size(axis), x.shape[dim])
        up = [(i, (i + 1) % size) for i in range(size - 1)]
        last = lax.slice_in_dim(x, length - width, length, axis=dim)
        leading = lax.slice_in_dim(x, 0, width, axis=dim)
        edges[dim] = (
            lax.ppermute(last, axis, up),
            lax.ppermute(leading, axis, [(b, a) for a, b in up]),
        )
    done = []
    for _, dim in sides:
        low, high = edges[dim]
        around = [(width, width) if d in done else (0, 0) for d in range(x.ndim)]
        x = jnp.concatenate([jnp.pad(low, around), x, jnp.pad(high, around)], axis=dim)
        done.append(dim)
    return x


def one_axis_at_a_time(x, axes):
    return functools.reduce(lax.psum, axes, x)


def stencil_step(padded, kappa_field):
    center = padded[1:-1, 1:-1]
    beside = padded[2:, 1:-1] + padded[:-2, 1:-1]
    beside = beside + padded[1:-1, 2:] + padded[1:-1, :-2]
    return (4.0 + kappa_field) * center - beside


def step_by_step(weight_field, response, kappa_field):
    def operate(field):
        first = extended(field, ((ROW, 0), (COL, 1)), 1)
        inner = stencil_step(first, kappa_field)
        second = extended(inner, ((ROW, 0), (COL, 1)), 1)
        return weight_field * field + smooth_weight * stencil_step(second, kappa_field)

    solution_field = jnp.zeros_like(response)
    residual = response

    def two_products(current, image):
        return (
            one_axis_at_a_time(jnp.sum(current * current), (ROW, COL)),
            one_axis_at_a_time(jnp.sum(current * image), (ROW, COL)),
        )

    image = operate(residual)
    norm_now, curvature = two_products(residual, image)
    alpha = norm_now / curvature
    direction, along = (residual, image)
    for step in range(ITERS):
        solution_field = solution_field + alpha * direction
        residual = residual - alpha * along
        if step + 1 < ITERS:
            image = operate(residual)
            norm_next, curvature = two_products(residual, image)
            ratio = norm_next / norm_now
            alpha = norm_next / (curvature - ratio * norm_next / alpha)
            direction = residual + ratio * direction
            along = image + ratio * along
            norm_now = norm_next
    return (solution_field, residual)


def per_device(obs_cell, obs_value, obs_weight, obs_count, kappa_field):
    rows, cols = lax.axis_size(ROW), lax.axis_size(COL)
    x, r, growth, weight_field, response = run(
        rows, cols, obs_cell[0], obs_value[0], obs_weight[0], obs_count[0], kappa_field
    )
    return lax.cond(
        growth[0, 0] <= GROWTH_MAX,
        lambda x, r, *rest: tuple(deliver(x, r)),
        lambda x, r, *rest: step_by_step(*rest),
        x, r, weight_field, response, kappa_field,
    )


def solution(mesh):
    placed = (
        P((ROW, COL), None, None, None),
        P((ROW, COL), None, None, None),
        P((ROW, COL), None, None, None),
        P((ROW, COL), None, None),
        P(ROW, COL),
    )
    return jax.shard_map(
        per_device,
        mesh=mesh,
        in_specs=placed,
        out_specs=(P(ROW, COL), P(ROW, COL)),
        check_vma=False,
    )
```

```python
import functools

import jax
import jax.numpy as jnp
from jax import lax
from jax.experimental import pallas as pl
from jax.experimental.pallas import tpu as pltpu
from jax.sharding import PartitionSpec as P

TILE = 128
ITERS = 3
ROW = "row"
COL = "col"
MESH = pl.DeviceIdType.MESH
LOGICAL = pl.DeviceIdType.LOGICAL
BF = jnp.bfloat16
F32 = jnp.float32
PITCH = 136
STRIDE = 5
GROUP = 16

smooth_weight = 0.05

SCALE = 1.0 / 256.0
SHIFT = 5.0
GROWTH_MAX = 1000.0
EDGE = 8
RIM = 6
WIDE = 128


def partner(me, devices, k):
    return lax.rem(me + STRIDE * k, devices)


def each_partner(devices, act):
    for k in range(1, 8):
        act(k)

    def some(g, _):
        for k in range(8):
            act(g * 8 + k)
        return 0

    lax.fori_loop(1, devices // 8, some, 0)


def exchange_and_bin(
    rows, cols, loads, ready, sent_out, cell_ref, value_ref, weight_ref, count_ref, wf_ref, resp_ref,
    stage_c, stage_w, stage_p, send_c, send_v, got_c, got_v,
    low_s, w_s, p_s, high_s, sent_c, sent_v, came_c, came_v,
):
    devices = rows * cols
    tiles = cell_ref.shape[0]
    me = lax.axis_index(ROW) * cols + lax.axis_index(COL)
    barrier = pltpu.get_barrier_semaphore()

    def greet(k):
        pl.semaphore_signal(
            barrier, inc=1, device_id=partner(me, devices, k), device_id_type=LOGICAL
        )

    each_partner(devices, greet)
    for copy in loads:
        copy.wait()

    counts = count_ref[...].T
    slot = lax.broadcasted_iota(jnp.int32, (devices, TILE), 1)
    for t in range(tiles):
        live = slot < jnp.broadcast_to(counts[:, t : t + 1], (devices, TILE))
        cell = cell_ref[t]
        code = jnp.bitwise_and(jnp.right_shift(cell, 13 + 6), 1) * 128 + jnp.bitwise_and(cell, 127)
        code = code * 64 + jnp.bitwise_and(jnp.right_shift(cell, 13), 63)
        wide = weight_ref[t].astype(F32)
        product = (wide * value_ref[t].astype(F32)).astype(BF).astype(F32)
        stage_c[pl.ds(t * PITCH, devices), :] = code
        stage_w[pl.ds(t * PITCH, devices), :] = jnp.where(live, wide, 0.0)
        stage_p[pl.ds(t * PITCH, devices), :] = jnp.where(live, product, 0.0)

    def gather(g, _):
        for j in range(8):
            k = g * 8 + j
            rows_at = pl.ds(partner(me, devices, k), tiles, stride=PITCH)
            send_c[k] = stage_c[rows_at, :].astype(jnp.int16)
            send_v[k, 0:16, :] = stage_w[rows_at, :].astype(BF)
            send_v[k, 16:32, :] = stage_p[rows_at, :].astype(BF)
        return 0

    lax.fori_loop(0, devices // 8, gather, 0)
    ready()
    pl.semaphore_wait(barrier, devices - 1)

    def send(k):
        to = partner(me, devices, k)
        pltpu.make_async_remote_copy(
            send_c.at[k], got_c.at[k], sent_c, came_c.at[k // GROUP], device_id=to, device_id_type=LOGICAL
        ).start()
        pltpu.make_async_remote_copy(
            send_v.at[k], got_v.at[k], sent_v, came_v.at[k // GROUP], device_id=to, device_id_type=LOGICAL
        ).start()

    each_partner(devices, send)
    sent_out()
    got_c[0] = send_c[0]
    got_v[0] = send_v[0]
    wf_ref[...] = jnp.zeros_like(wf_ref)
    resp_ref[...] = jnp.zeros_like(resp_ref)

    lanes = lax.broadcasted_iota(jnp.int32, (16, 128), 1).astype(F32)
    high_ids = [lanes.astype(BF), (lanes + 128.0).astype(BF)]
    subs = lax.broadcasted_iota(jnp.int32, (16, 128), 0).astype(F32)
    low_ids = [(subs + 16.0 * g).astype(BF) for g in range(4)]
    one, zero = jnp.ones((16, 128), BF), jnp.zeros((16, 128), BF)
    across = wf_ref.shape[1] // TILE

    def bin_group(g):
        code = got_c[pl.ds(g * GROUP, GROUP)].reshape(GROUP * tiles, 128).astype(jnp.int32)
        low_s[...] = jnp.bitwise_and(code, 63).astype(F32)
        high_s[...] = jnp.right_shift(code, 6).astype(F32)
        for s in range(GROUP):
            w_s[pl.ds(s * 16, 16), :] = got_v[g * GROUP + s, 0:16, :].astype(F32)
            p_s[pl.ds(s * 16, 16), :] = got_v[g * GROUP + s, 16:32, :].astype(F32)
        for t in range(tiles):
            total = None
            for pair in range(GROUP // 2):
                left, right = [], []
                for s in (2 * pair, 2 * pair + 1):
                    r = s * 16 + t
                    low, high, w, p = (
                        jnp.broadcast_to(ref[pl.ds(r, 1), :], (16, 128)).astype(BF)
                        for ref in (low_s, high_s, w_s, p_s)
                    )
                    hits = [low == ids for ids in low_ids]
                    left.append(
                        jnp.concatenate(
                            [jnp.where(h, w, zero) for h in hits]
                            + [jnp.where(h, p, zero) for h in hits],
                            axis=0,
                        )
                    )
                    turned = jnp.concatenate([high] * 8, axis=0).T
                    for v in range(8):
                        part = turned[16 * v : 16 * v + 16]
                        right.append(
                            jnp.concatenate([jnp.where(part == ids, one, zero) for ids in high_ids], axis=1)
                        )
                piece = jnp.dot(
                    jnp.concatenate(left, axis=1),
                    jnp.concatenate(right, axis=0),
                    preferred_element_type=F32,
                )
                total = piece if total is None else total + piece
            for ref, at in ((wf_ref, 0), (resp_ref, 64)):
                for half in range(2):
                    where = (
                        pl.ds((t // across) * TILE + half * 64, 64),
                        pl.ds((t % across) * TILE, TILE),
                    )
                    ref[where] = ref[where] + total[at : at + 64, half * 128 : half * 128 + 128]

    def arrived(first, size, g):
        there = pl.ds(first, size)
        pltpu.make_async_copy(got_c.at[there], got_c.at[there], came_c.at[g]).wait()
        pltpu.make_async_copy(got_v.at[there], got_v.at[there], came_v.at[g]).wait()

    def step(g, _):
        @pl.when(g == 0)
        def _():
            arrived(1, GROUP - 1, 0)

        @pl.when(g > 0)
        def _():
            arrived(g * GROUP, GROUP, g)

        bin_group(g)
        return 0

    lax.fori_loop(0, devices // GROUP, step, 0)
    out = pl.ds(1, devices - 1)
    pltpu.make_async_copy(send_c.at[out], send_c.at[out], sent_c).wait()
    pltpu.make_async_copy(send_v.at[out], send_v.at[out], sent_v).wait()


def solve(m):
    shift = SCALE * SHIFT

    def at(p, i):
        return p[i] if 0 <= i < len(p) else None

    def plus(a, b):
        return b if a is None else a if b is None else a + b

    def dot(a, b):
        total, size = None, None
        for i, x in enumerate(a):
            for j, y in enumerate(b):
                term = x * y * m[i + j]
                total, size = plus(total, term), plus(size, jnp.abs(term))
        return total, size / jnp.abs(total)

    def times_a(p):
        out = []
        for i in range(len(p) + 1):
            scaled = None if at(p, i) is None else shift * p[i]
            out.append(plus(scaled, at(p, i - 1)))
        return out

    def axpy(a, b, c):
        return [
            plus(at(a, i), None if at(b, i) is None else c * b[i]) for i in range(max(len(a), len(b)))
        ]

    one = jnp.ones_like(m[0])
    x, r, p, rr, growth = [], [one], [one], m[0], one
    for step in range(ITERS):
        ap = times_a(p)
        pap, grown = dot(p, ap)
        growth = jnp.where(grown <= growth, growth, grown)
        alpha = rr / pap
        x, r = axpy(x, p, alpha), axpy(r, ap, -alpha)
        if step + 1 < ITERS:
            new, grown = dot(r, r)
            growth = jnp.where(grown <= growth, growth, grown)
            p, rr = axpy(r, p, new / rr), new
    return x, r, growth


class Edges:
    def __init__(self, rows, cols, rows_out, cols_out, rows_in, cols_in, corners, sent, came):
        row, col = lax.axis_index(ROW), lax.axis_index(COL)
        above, below = lax.rem(row + rows - 1, rows), lax.rem(row + 1, rows)
        before, after = lax.rem(col + cols - 1, cols), lax.rem(col + 1, cols)
        self.rows_out, self.cols_out = rows_out, cols_out
        self.rows_in, self.cols_in, self.corners = rows_in, cols_in, corners
        last = cols_out.shape[2] - 1
        plan = [
            (rows_out.at[0], rows_in.at[1], above, col),
            (rows_out.at[1], rows_in.at[0], below, col),
            (cols_out.at[0], cols_in.at[1], row, before),
            (cols_out.at[1], cols_in.at[0], row, after),
            (cols_out.at[0, :, 0], corners.at[3], above, before),
            (cols_out.at[0, :, last], corners.at[1], below, before),
            (cols_out.at[1, :, 0], corners.at[2], above, after),
            (cols_out.at[1, :, last], corners.at[0], below, after),
        ]
        self.copies = [
            pltpu.make_async_remote_copy(
                source, target, sent.at[i], came.at[i], device_id=(pr, pc), device_id_type=MESH
            )
            for i, (source, target, pr, pc) in enumerate(plan)
        ]

    def start(self):
        for copy in self.copies:
            copy.start()

    def wait(self):
        for copy in self.copies:
            copy.wait()


def lay_out(ref, field):
    high, wide = field.shape
    strip = high // 8
    for s in range(8):
        for j in range(wide // WIDE):
            ref[j, pl.ds(RIM * 8 + s, strip, stride=8), :] = field[s * strip : (s + 1) * strip, j * WIDE : (j + 1) * WIDE]


def group(i, n=1):
    return pl.ds(i * 8, n * 8)


def pack_edges(ref, f, edges, top, bottom):
    lane = lax.broadcasted_iota(jnp.int32, (8, WIDE), 1)
    tiles = ref.shape[0] - 1
    edges.rows_out[0, f] = top
    edges.rows_out[1, f] = bottom
    for q in range(edges.cols_out.shape[2]):
        left, right = jnp.zeros((8, WIDE), F32), jnp.zeros((8, WIDE), F32)
        for n in range(16):
            slot = (lane >= 8 * n) & (lane < 8 * n + 8)
            at = group(RIM + 16 * q + n)
            left = jnp.where(slot, pltpu.roll(ref[0, at, :], 8 * n, 1), left)
            right = jnp.where(slot, pltpu.roll(ref[tiles - 1, at, :], (8 * n + 8) % WIDE, 1), right)
        edges.cols_out[0, f, q] = left
        edges.cols_out[1, f, q] = right


def fill_edges(ref, f, edges, keep):
    lane = lax.broadcasted_iota(jnp.int32, (8, WIDE), 1)
    sub = lax.broadcasted_iota(jnp.int32, (8, WIDE), 0)
    tiles = ref.shape[0] - 1
    strip = ref.shape[1] // 8 - 2 * RIM
    above, below, before, after = keep

    def beside(left, right, n):
        left = pltpu.roll(left, (120 - 8 * n) % WIDE, 1)
        right = pltpu.roll(right, (WIDE - 8 * n) % WIDE, 1)
        return jnp.where(lane < 8, right * after, jnp.where(lane >= 120, left * before, 0.0))

    for i in range(strip):
        q, n = i // 16, i % 16
        ref[tiles, group(RIM + i), :] = beside(edges.cols_in[0, f, q], edges.cols_in[1, f, q], n)
    for j in range(tiles + 1):
        for i in range(RIM):
            if j < tiles:
                up = edges.rows_in[0, f, EDGE - RIM + i : EDGE - RIM + i + 1, j * WIDE : (j + 1) * WIDE]
                down = edges.rows_in[1, f, i : i + 1, j * WIDE : (j + 1) * WIDE]
                up, down = (jnp.broadcast_to(x, (8, WIDE)) for x in (up, down))
            else:
                up = beside(edges.corners[0, f], edges.corners[1, f], 16 - RIM + i)
                down = beside(edges.corners[2, f], edges.corners[3, f], i)
                up, down = pltpu.roll(up, 1, 0), pltpu.roll(down, 7, 0)
            inside = pltpu.roll(ref[j, group(strip + i), :], 1, 0)
            ref[j, group(i), :] = jnp.where(sub == 0, up * above, inside)
            inside = pltpu.roll(ref[j, group(RIM + i), :], 7, 0)
            ref[j, group(RIM + strip + i), :] = jnp.where(sub == 7, down * below, inside)


def smooth(
    rows, cols, while_waiting, early, middle, late, wf_ref, resp_ref, x_ref, r_ref, growth_ref,
    v0, v1, v2, v3, u, w, c, y1, y2, y3, part, parts, sent_part, came_part,
):
    devices = rows * cols
    high, wide = x_ref.shape
    tiles, strip = wide // WIDE, high // 8
    row, col = lax.axis_index(ROW), lax.axis_index(COL)
    me = row * cols + col
    keep = tuple(
        jnp.where(there, 1.0, 0.0).astype(F32)
        for there in (row > 0, row < rows - 1, col > 0, col < cols - 1)
    )

    first, last = slice(0, EDGE), slice(high - EDGE, high)
    lay_out(v0, resp_ref[...])
    pack_edges(v0, 0, middle, resp_ref[first, :], resp_ref[last, :])
    middle.start()
    lay_out(w, (wf_ref[...] - SHIFT) * SCALE)
    pack_edges(w, 0, late, (wf_ref[first, :] - SHIFT) * SCALE, (wf_ref[last, :] - SHIFT) * SCALE)
    late.start()
    early.wait()
    fill_edges(c, 0, early, (1.0,) * 4)
    middle.wait()
    fill_edges(v0, 0, middle, keep)

    lane = lax.broadcasted_iota(jnp.int32, (8, WIDE), 1)
    sub = lax.broadcasted_iota(jnp.int32, (8, WIDE), 0)
    side = jnp.where(lane < 64, keep[3], keep[2])
    upper = jnp.where(sub == 0, keep[0], 1.0)
    lower = jnp.where(sub == 7, keep[1], 1.0)

    def laplace(ref, i, n):
        size = n * 8
        lanes = lax.broadcasted_iota(jnp.int32, (size, WIDE), 1)
        tall = [ref[j, group(i - 1, n + 2), :] for j in range(tiles + 1)]
        here = [x[8 : 8 + size] for x in tall]
        later = [pltpu.roll(x, 1, 1) for x in here]
        sooner = [pltpu.roll(x, WIDE - 1, 1) for x in here]
        out = []
        for j in range(tiles + 1):
            left = jnp.where(lanes == 0, later[j - 1], later[j])
            right = jnp.where(lanes == WIDE - 1, sooner[(j + 1) % (tiles + 1)], sooner[j])
            beside = (tall[j][0:size] + tall[j][16 : 16 + size]) + (left + right)
            out.append(c[j, group(i, n), :] * here[j] - beside)
        return out, here

    def masked(x, n, j, edge):
        if edge is not None:
            x = x * jnp.concatenate([edge] * n, axis=0)
        if j == tiles:
            x = x * jnp.concatenate([side] * n, axis=0)
        return x

    def inner(ref, i, n, edge=None):
        news, olds = laplace(ref, i, n)
        news = [masked(x, n, j, edge) for j, x in enumerate(news)]
        for j, x in enumerate(news):
            u[j, group(i, n), :] = x
        return news[:tiles], olds[:tiles]

    def outer(ref, out, i, n, edge=None):
        news, olds = [], []
        for j, x in enumerate(laplace(u, i, n)[0]):
            old = ref[j, group(i, n), :]
            new = masked(w[j, group(i, n), :] * old + (smooth_weight * SCALE) * x, n, j, edge)
            out[j, group(i, n), :] = new
            news.append(new)
            olds.append(old)
        return news[:tiles], olds[:tiles]

    def fold(pairs, n):
        total = None
        for a, b in pairs:
            product = a * b
            for i in range(n):
                piece = product[i * 8 : i * 8 + 8]
                total = piece if total is None else total + piece
        return total

    n = 32
    zero = jnp.zeros((8, WIDE), F32)
    moments = []
    for step, (ref, out) in enumerate(((v0, v1), (v1, v2), (v2, v3))):
        rim = RIM - 1 - 2 * step
        inner(ref, RIM - rim, rim, upper)
        inner(ref, RIM + strip, rim, lower)

        def rows_of_u(k, sums, ref=ref, step=step):
            news, olds = inner(ref, RIM + k * n, n)
            if step < 2:
                return sums
            weighted = [w[j, group(RIM + k * n, n), :] * x for j, x in enumerate(olds)]
            return sums[0] + fold(zip(weighted, olds), n), sums[1] + fold(zip(news, news), n)

        sums = lax.fori_loop(0, strip // n, rows_of_u, (zero,) * (0, 0, 2)[step])
        if step == 2:
            moments.append(sums[0] + (smooth_weight * SCALE) * sums[1])
            break
        if step == 0:
            late.wait()
            fill_edges(w, 0, late, (1.0,) * 4)
        outer(ref, out, RIM - rim + 1, rim - 1, upper)
        outer(ref, out, RIM + strip, rim - 1, lower)

        def rows_of_v(k, sums, ref=ref, out=out, step=step):
            news, olds = outer(ref, out, RIM + k * n, n)
            terms = [fold(zip(olds, news), n), fold(zip(news, news), n)]
            if step == 0:
                terms.append(fold(zip(olds, olds), n))
            return tuple(s + t for s, t in zip(sums, terms))

        sums = lax.fori_loop(0, strip // n, rows_of_v, (zero,) * (3, 2)[step])
        moments += [sums[2], sums[0], sums[1]] if step == 0 else list(sums)

    column = lax.broadcasted_iota(jnp.int32, (1, WIDE), 1)
    mine = jnp.zeros((1, WIDE), F32)
    for j, m in enumerate(moments):
        mine = mine + jnp.where(column == j, jnp.sum(jnp.sum(m, axis=0, keepdims=True), axis=1, keepdims=True), 0.0)
    part[...] = mine
    parts[me] = mine

    def tell(k):
        to = partner(me, devices, k)
        pltpu.make_async_remote_copy(
            part, parts.at[me], sent_part, came_part, device_id=to, device_id_type=LOGICAL
        ).start()

    each_partner(devices, tell)
    while_waiting()

    def rows_of_last(k, _):
        outer(v2, v3, RIM + k * n, n)
        return 0

    lax.fori_loop(0, strip // n, rows_of_last, 0)

    def straighten(s, _):
        for j in range(tiles):
            place = (pl.ds(s * strip, strip), pl.ds(j * WIDE, WIDE))
            for ref, flat in ((v1, y1), (v2, y2), (v3, y3)):
                flat[place] = ref[j, pl.ds(RIM * 8 + s, strip, stride=8), :]
        return 0

    lax.fori_loop(0, 8, straighten, 0)
    others = pl.ds(1, devices - 1)
    pltpu.make_async_copy(parts.at[others], parts.at[others], came_part).wait()
    total = jnp.sum(parts[...], axis=0)
    m = [jnp.sum(jnp.where(column == j, total, 0.0), axis=1, keepdims=True) for j in range(len(moments))]
    xs, rs, growth = solve([jnp.broadcast_to(value, (1, WIDE)) for value in m])
    growth_ref[...] = growth

    def spread(value):
        return jnp.concatenate([jnp.broadcast_to(value, (128, WIDE))] * tiles, axis=1)

    def combine(k, _):
        at = pl.ds(k * 128, 128)
        basis = [ref[at, :] for ref in (resp_ref, y1, y2, y3)]
        x_ref[at, :] = sum(spread(a * SCALE) * v for a, v in zip(xs, basis))
        r_ref[at, :] = sum(spread(a) * v for a, v in zip(rs, basis))
        return 0

    lax.fori_loop(0, high // 128, combine, 0)
    pltpu.make_async_copy(parts.at[others], parts.at[others], sent_part).wait()


def whole(rows, cols, *refs):
    inputs, (x, r, growth, *kept), inside, (wf, resp) = refs[:5], refs[5:10], refs[10:15], refs[15:17]
    first, second, moved = refs[17:32], refs[32:46], refs[67]
    early, middle, late = (Edges(rows, cols, *refs[i : i + 7]) for i in (46, 53, 60))
    kappa, c = inside[4], second[6]
    loads = [pltpu.make_async_copy(a, b, moved.at[i]) for i, (a, b) in enumerate(zip(inputs, inside))]
    for copy in loads:
        copy.start()
    stores = [pltpu.make_async_copy(a, b, moved.at[5 + i]) for i, (a, b) in enumerate(zip((wf, resp), kept))]

    def ready():
        loads[4].wait()
        lay_out(c, kappa[...] + 4.0)
        high = kappa.shape[0]
        pack_edges(c, 0, early, kappa[0:EDGE, :] + 4.0, kappa[high - EDGE : high, :] + 4.0)

    exchange_and_bin(rows, cols, loads[:4], ready, early.start, *inside[:4], wf, resp, *first)

    def while_waiting():
        for copy in stores:
            copy.start()

    smooth(rows, cols, while_waiting, early, middle, late, wf, resp, x, r, growth, *second)
    for copy in stores:
        copy.wait()


def hand_over(*refs):
    copies = [pltpu.make_async_copy(refs[i], refs[2 + i], refs[4].at[i]) for i in range(2)]
    for copy in copies:
        copy.start()
    for copy in copies:
        copy.wait()


def deliver(x, r):
    return pl.pallas_call(
        hand_over,
        out_shape=[jax.ShapeDtypeStruct(a.shape, a.dtype) for a in (x, r)],
        in_specs=[pl.BlockSpec(memory_space=pl.ANY)] * 2,
        out_specs=[pl.BlockSpec(memory_space=pltpu.HBM)] * 2,
        scratch_shapes=[pltpu.SemaphoreType.DMA((2,))],
        name="deliver",
    )(x, r)


def run(rows, cols, obs_cell, obs_value, obs_weight, obs_count, kappa_field):
    devices = rows * cols
    tiles = obs_cell.shape[0]
    high, wide = kappa_field.shape
    arguments = (obs_cell, obs_value, obs_weight, obs_count, kappa_field)
    vmem = pl.BlockSpec(memory_space=pltpu.VMEM)
    hbm = pl.BlockSpec(memory_space=pltpu.HBM)
    stage = (tiles * PITCH, TILE)
    work = pltpu.VMEM((wide // WIDE + 1, (high // 8 + 2 * RIM) * 8, WIDE), F32)

    def edges(count):
        ends = pltpu.VMEM((2, count, EDGE, wide), F32)
        sides = pltpu.VMEM((2, count, high // WIDE, 8, WIDE), F32)
        return [ends, sides, ends, sides, pltpu.VMEM((4, count, 8, WIDE), F32), dma((8,)), dma((8,))]

    dma = pltpu.SemaphoreType.DMA
    shape = jax.ShapeDtypeStruct((high, wide), F32)
    return pl.pallas_call(
        functools.partial(whole, rows, cols),
        out_shape=[pltpu.VMEM((high, wide), F32), pltpu.VMEM((high, wide), F32), pltpu.VMEM((1, WIDE), F32), shape, shape],
        in_specs=[hbm] * 5,
        out_specs=[vmem] * 3 + [hbm] * 2,
        scratch_shapes=[
            *[pltpu.VMEM(a.shape, a.dtype) for a in arguments],
            pltpu.VMEM((high, wide), F32),
            pltpu.VMEM((high, wide), F32),
            pltpu.VMEM(stage, jnp.int32),
            pltpu.VMEM(stage, F32),
            pltpu.VMEM(stage, F32),
            pltpu.VMEM((devices, tiles, TILE), jnp.int16),
            pltpu.VMEM((devices, 2 * tiles, TILE), BF),
            pltpu.VMEM((devices, tiles, TILE), jnp.int16),
            pltpu.VMEM((devices, 2 * tiles, TILE), BF),
            *[pltpu.VMEM((GROUP * tiles, TILE), F32)] * 4,
            dma,
            dma,
            dma((devices // GROUP,)),
            dma((devices // GROUP,)),
            *[work] * 7,
            *[pltpu.VMEM((high, wide), F32)] * 3,
            pltpu.VMEM((1, WIDE), F32),
            pltpu.VMEM((devices, 1, WIDE), F32),
            dma,
            dma,
            *edges(1),
            *edges(1),
            *edges(1),
            dma((7,)),
        ],
        name="bin_and_smooth",
        compiler_params=pltpu.CompilerParams(collective_id=0, has_side_effects=True),
    )(*arguments)


def extended(x, sides, width):
    edges = {}
    for axis, dim in sides:
        size, length = (lax.axis_size(axis), x.shape[dim])
        up = [(i, (i + 1) % size) for i in range(size - 1)]
        last = lax.slice_in_dim(x, length - width, length, axis=dim)
        leading = lax.slice_in_dim(x, 0, width, axis=dim)
        edges[dim] = (
            lax.ppermute(last, axis, up),
            lax.ppermute(leading, axis, [(b, a) for a, b in up]),
        )
    done = []
    for _, dim in sides:
        low, high = edges[dim]
        around = [(width, width) if d in done else (0, 0) for d in range(x.ndim)]
        x = jnp.concatenate([jnp.pad(low, around), x, jnp.pad(high, around)], axis=dim)
        done.append(dim)
    return x


def one_axis_at_a_time(x, axes):
    return functools.reduce(lax.psum, axes, x)


def stencil_step(padded, kappa_field):
    center = padded[1:-1, 1:-1]
    beside = padded[2:, 1:-1] + padded[:-2, 1:-1]
    beside = beside + padded[1:-1, 2:] + padded[1:-1, :-2]
    return (4.0 + kappa_field) * center - beside


def step_by_step(weight_field, response, kappa_field):
    def operate(field):
        first = extended(field, ((ROW, 0), (COL, 1)), 1)
        inner = stencil_step(first, kappa_field)
        second = extended(inner, ((ROW, 0), (COL, 1)), 1)
        return weight_field * field + smooth_weight * stencil_step(second, kappa_field)

    solution_field = jnp.zeros_like(response)
    residual = response

    def two_products(current, image):
        return (
            one_axis_at_a_time(jnp.sum(current * current), (ROW, COL)),
            one_axis_at_a_time(jnp.sum(current * image), (ROW, COL)),
        )

    image = operate(residual)
    norm_now, curvature = two_products(residual, image)
    alpha = norm_now / curvature
    direction, along = (residual, image)
    for step in range(ITERS):
        solution_field = solution_field + alpha * direction
        residual = residual - alpha * along
        if step + 1 < ITERS:
            image = operate(residual)
            norm_next, curvature = two_products(residual, image)
            ratio = norm_next / norm_now
            alpha = norm_next / (curvature - ratio * norm_next / alpha)
            direction = residual + ratio * direction
            along = image + ratio * along
            norm_now = norm_next
    return (solution_field, residual)


def per_device(obs_cell, obs_value, obs_weight, obs_count, kappa_field):
    rows, cols = lax.axis_size(ROW), lax.axis_size(COL)
    x, r, growth, weight_field, response = run(
        rows, cols, obs_cell[0], obs_value[0], obs_weight[0], obs_count[0], kappa_field
    )
    return lax.cond(
        growth[0, 0] <= GROWTH_MAX,
        lambda x, r, *rest: tuple(deliver(x, r)),
        lambda x, r, *rest: step_by_step(*rest),
        x, r, weight_field, response, kappa_field,
    )


def solution(mesh):
    placed = (
        P((ROW, COL), None, None, None),
        P((ROW, COL), None, None, None),
        P((ROW, COL), None, None, None),
        P((ROW, COL), None, None),
        P(ROW, COL),
    )
    return jax.shard_map(
        per_device,
        mesh=mesh,
        in_specs=placed,
        out_specs=(P(ROW, COL), P(ROW, COL)),
        check_vma=False,
    )
```
